256 devices in a mesh: groups: 2 (over y), heads: 32 (over z, core), batch: 4 (over x).
Axes of the slice: x: 4, y: 2, z: 16, core: 2. Of those that a mesh axis runs over, the one named last changes fastest.
The devices are a block of a 4x16x16 slice.
Arguments:
- queries: bfloat16 [128, 8192], P(('groups', 'batch'), 'heads'), parts along dimension 0, may hold values from -110 to 110
- new_kv: bfloat16 [64, 64, 256], P(('groups', 'heads'), 'batch'), parts along dimension 0, may hold values from -15 to 15
- kv_pool: bfloat16 [64, 192, 128, 256], P(('groups', 'heads'), 'batch'), parts along dimension 0, may hold values from -6 to 6
- page_counts: int32 [8, 16], P(('groups', 'batch')), parts along dimension 0, may hold values from 1 to 6, 48 in all within a row
- last_fill: int32 [8, 16], P(('groups', 'batch')), parts along dimension 0, may hold values from 1 to 128
- page_order: int32 [8, 48], P(('groups', 'batch')), parts along dimension 0, may hold values from 0 to 47, each once within a row
- hidden: bfloat16 [128, 8192], P(('groups', 'batch')), parts along dimension 0, may hold values from -0.59765625 to 0.59765625
- out_weight: bfloat16 [8192, 8192], P('heads'), may hold values from -0.5 to 0.5
- norm_gain: bfloat16 [8192], replicated, may hold values from 0.099609375 to 1.8984375
- sectioned: bfloat16 [64, 4, 8, 128, 256], P(('groups', 'heads'), 'batch'), parts along dimension 0, may hold values from -6 to 6
- routes: int32 [64, 4, 8, 1], P(('groups', 'heads'), 'batch'), parts along dimension 0, may hold values from 0 to 7; in each aligned block of 8 rows (0 to 7, 8 to 15, ..., all dimensions but the last counted through in order) at most 2 rows name the same one
Outputs:
- residual_out: bfloat16 [128, 8192], P(('groups', 'batch')), parts along dimension 0
- normed: bfloat16 [128, 8192], P(('groups', 'batch')), parts along dimension 0
- arrival: bfloat16 [64, 4, 32, 2, 128, 256], P(('groups', 'heads'), 'batch'), parts along dimension 0
The draws below stay inside these ranges and needn't reach their ends.
There are 2 independent parts, one for each index of `groups`. The reference program is written for one: setup_inputs(seed, part) draws one part's arguments, and reference() takes and returns one part's arrays. A program takes and returns all parts, laid end to end along the dimension named above; an argument that names none is the same for every part. Nothing has to cross between parts.
Inputs may be any that keep to these rules, and one draw needn't show every extreme that they name: `routes`: every key-value head is named by at most 2 sectioned pages of one device. `page_counts`: the page counts of one batch owner sum to 48.
All inputs are finite; a program needn't handle non-finite values.
Results may differ from the reference program's by a relative error of at most 0.0066.
Values may be sent and summed in bfloat16 or wider, within the bound.
A program may use at most 64 MiB of HBM per device.

```python
import math
import jax
import jax.numpy as jnp
import numpy as np
from jax import lax

D = 8192
Q_HEADS = 64
KV_HEADS = 8
HEAD_DIM = 128
PAGE = 128
MAX_PAGES = 6
SECTION_DEV = 8
PER_HEAD_CAP = 2
REQ_DEV = 16
KV_WIDTH = 256
CACHE_SLOTS = 32
POOL_DEV = 48
REQUESTS = 64
N_HEADS = 32
N_BATCH = 4


def draw_kv_pool(key, part):
    full_shape = (CACHE_SLOTS, N_BATCH * POOL_DEV, PAGE, 2 * HEAD_DIM)
    base_draw = jnp.clip(jax.random.normal(jax.random.fold_in(key, 101), full_shape, jnp.float32), -6.0, 6.0)
    return base_draw.astype(jnp.bfloat16)


def draw_queries(key, part):
    row_total = N_BATCH * REQ_DEV
    base_draw = jnp.clip(jax.random.normal(jax.random.fold_in(key, 201), (row_total, Q_HEADS, HEAD_DIM), jnp.float32), -6.0, 6.0)
    return base_draw.reshape(row_total, Q_HEADS * HEAD_DIM).astype(jnp.bfloat16)


def draw_out_weight(key, part):
    row_total = Q_HEADS * HEAD_DIM
    common_share = 0.2
    scale_reach = 0.6
    base_draw = jnp.clip(jax.random.normal(jax.random.fold_in(key, 301), (row_total, D), jnp.float32), -4.0, 4.0)
    loadings = jnp.clip(jax.random.normal(jax.random.fold_in(key, 302), (row_total, 1), jnp.float32), -3.0, 3.0)
    common_row = jnp.clip(jax.random.normal(jax.random.fold_in(key, 303), (1, D), jnp.float32), -3.0, 3.0)
    row_scale = jnp.exp(jax.random.uniform(jax.random.fold_in(key, 304), (row_total, 1), jnp.float32, -scale_reach, scale_reach))
    row_scale = row_scale / math.sqrt(math.sinh(2.0 * scale_reach) / (2.0 * scale_reach))
    mixed_rows = math.sqrt(1.0 - common_share) * base_draw + math.sqrt(common_share) * loadings * common_row
    weights = row_scale * mixed_rows / math.sqrt(row_total)
    return weights.astype(jnp.bfloat16)


def with_ends(array, stream_key, smallest, high):
    index_at = [jax.random.randint(jax.random.fold_in(stream_key, axis), (), 0, length) for axis, length in enumerate(array.shape)]
    longest = array.shape.index(max(array.shape))
    neighbour = index_at[:longest] + [(index_at[longest] + 1) % array.shape[longest]] + index_at[longest + 1:]
    return array.at[tuple(index_at)].set(smallest).at[tuple(neighbour)].set(high)


def block_scale(rng, shape, cuts, smallest, high):
    def one(dim, blocks):
        heights = jax.random.uniform(jax.random.fold_in(jax.random.fold_in(rng, 6), dim), (blocks,), jnp.float32, smallest / len(cuts), high / len(cuts))
        return jnp.repeat(jnp.exp(heights), shape[dim] // blocks).reshape((-1,) + (1,) * (len(shape) - dim - 1))

    loudness = one(*cuts[0])
    for cut in cuts[1:]:
        loudness = loudness * one(*cut)
    return loudness


def length_profile(number_of, total, reach, skew):
    portions = [(1 << 20) // math.isqrt(grade ** skew) + 1 for grade in range(2, number_of + 1)]
    spare, given = total - reach - (number_of - 1), [1] * (number_of - 1)
    while spare > 0:
        free = [i for i in range(number_of - 1) if given[i] < reach]
        pool, left = sum([portions[i] for i in free]), spare
        for i in free:
            addition = min(reach - given[i], max(1, left * portions[i] // pool), spare)
            given[i] = given[i] + addition
            spare = spare - addition
    return np.array([reach] + given)


def uneven_parts(stream_key, number_of, total, reach, lean):
    if number_of == 2:
        one = jax.random.randint(stream_key, (), max(1, total - reach), min(reach, total - 1) + 1)
        return jnp.stack([one, total - one])
    tallies = jnp.asarray(length_profile(number_of, total, reach, lean), jnp.int32)
    twos = (number_of - 1) // 2
    source_of, sink = tallies[1:1 + 2 * twos:2], tallies[2:2 + 2 * twos:2]
    slack = jnp.minimum(source_of - 1, reach - sink)
    shifted = jax.random.randint(jax.random.fold_in(stream_key, 1), (twos,), 0, 1 << 20) % (slack + 1)
    tallies = tallies.at[1:1 + 2 * twos:2].set(source_of - shifted).at[2:2 + 2 * twos:2].set(sink + shifted)
    return tallies[jax.random.permutation(jax.random.fold_in(stream_key, 2), number_of)]


def deal_out(own_key, own, number, rows, amount, top, reach, lean):
    sequence = jax.random.permutation(own_key, amount)
    crowded, ordinary = shares(amount, rows * top, reach, lean, True), shares(amount, rows * top, reach, lean, False)
    places = jnp.arange(amount)

    def named(sizes, rotation):
        used = int((sizes > 0).sum())
        fixed = max(1, used // 4)
        moved = fixed + (places - fixed + rotation * (used - fixed)) % max(1, amount - fixed)
        return jnp.zeros((amount,), jnp.int32).at[sequence[jnp.where(places < fixed, places, moved)]].set(jnp.asarray(sizes, jnp.int32))

    sizes = jnp.where(number % 4 == 0, named(crowded, number // 4), named(ordinary, number - number // 4 - 1))
    mixed = jax.random.permutation(jax.random.fold_in(own, 3), amount)
    giver, taker = mixed[0:amount // 2 * 2:2], mixed[1:amount // 2 * 2:2]
    room = jnp.minimum(sizes[giver] - 1, reach - sizes[taker]) // 2
    room = jnp.where((giver == sequence[0]) | (taker == sequence[0]) | (sizes[taker] == 0), 0, jnp.maximum(room, 0))
    moved = jax.random.randint(jax.random.fold_in(own, 4), (amount // 2,), 0, 1 << 20) % (room + 1)
    sizes = sizes.at[giver].add(-moved).at[taker].add(moved)
    members = jnp.searchsorted(jnp.cumsum(sizes), jnp.arange(rows * top), side="right").astype(jnp.int32)
    table = members.reshape(top, rows).T
    table = table[jax.random.permutation(jax.random.fold_in(own, 1), rows)]
    rotation = jax.random.randint(jax.random.fold_in(own, 2), (rows, 1), 0, top)
    return jnp.take_along_axis(table, (jnp.arange(top)[None, :] + rotation) % top, axis=1)


def shares(amount, total, limit, slope, full):
    loads = [(1 << 20) // math.isqrt(grade ** slope) + 1 for grade in range(1, amount + 1)]
    largest = limit if full else min(limit, max(-(-total // amount), total * loads[0] // sum(loads)))
    least = 1 if total - largest >= amount - 1 else 0
    holding, spare = [largest] + [least] * (amount - 1), total - largest - least * (amount - 1)
    while spare > 0:
        candidates = [i for i in range(1, amount) if holding[i] < largest] or [i for i in range(1, amount) if holding[i] < limit]
        pool, remaining = sum([loads[i] for i in candidates]), spare
        for i in candidates:
            addition = min(limit - holding[i], max(1, remaining * loads[i] // pool), spare)
            holding[i] = holding[i] + addition
            spare = spare - addition
    return np.array(holding)


def centred(key, dims, spread, bound, split=(), kind=jnp.bfloat16):
    values = jax.random.normal(key, dims, jnp.float32) * spread
    if len(split) > 0:
        values = block_scale(key, dims, split, -0.22, 0.18) * values
    return jnp.clip(values, min=-bound, max=bound).astype(kind)


def setup_inputs(seed: int = 0, part: int = 0) -> dict:
    splits = jax.random.split(jax.random.key(seed), 12)
    part_keys = jax.random.split(jax.random.fold_in(splits[11], part), 12)
    queries = draw_queries(jax.random.fold_in(jax.random.fold_in(splits[11], part), 71), part)
    new_kv = centred(part_keys[1], (CACHE_SLOTS, REQUESTS, KV_WIDTH), 2.5, 15.0, ((0, 32), (1, 4)))
    kv_pool = draw_kv_pool(jax.random.fold_in(jax.random.fold_in(splits[11], part), 71), part)
    page_counts = jax.vmap(lambda own: uneven_parts(own, REQ_DEV, POOL_DEV, MAX_PAGES, 1))(jax.random.split(part_keys[3], N_BATCH)).reshape((N_BATCH, REQ_DEV)).astype(jnp.int32)
    last_fill = with_ends(jax.random.randint(part_keys[4], (N_BATCH, REQ_DEV), 1, PAGE + 1), jax.random.fold_in(part_keys[4], 1), 1, PAGE).astype(jnp.int32)
    page_order = jax.vmap(lambda own: jax.random.permutation(own, POOL_DEV))(jax.random.split(part_keys[5], N_BATCH)).reshape((N_BATCH, POOL_DEV)).astype(jnp.int32)
    hidden = centred(part_keys[6], (REQUESTS, D), 0.1, 0.59765625, ((0, 4),))
    out_weight = draw_out_weight(jax.random.fold_in(splits[11], 71), part)
    norm_gain = jnp.clip(1.0 + 0.18 * jax.random.normal(splits[8], (D,), jnp.float32), 0.099609375, 1.8984375).astype(jnp.bfloat16)
    sectioned = centred(part_keys[9], (N_HEADS, N_BATCH, SECTION_DEV, PAGE, KV_WIDTH), 1.0, 6.0, ((0, 32), (1, 4)))
    routes_keys = jax.random.split(jax.random.fold_in(part_keys[10], 1), N_HEADS * N_BATCH * SECTION_DEV // SECTION_DEV)
    routes_turns = jax.random.permutation(jax.random.fold_in(part_keys[10], 3), N_HEADS * N_BATCH * SECTION_DEV // SECTION_DEV)
    routes = jax.vmap(lambda own, number: deal_out(jax.random.fold_in(part_keys[10], 2), own, number, SECTION_DEV, KV_HEADS, 1, PER_HEAD_CAP, 2))(routes_keys, routes_turns).reshape((N_HEADS, N_BATCH, SECTION_DEV, 1))
    return {"queries": queries, "new_kv": new_kv, "kv_pool": kv_pool, "page_counts": page_counts, "last_fill": last_fill, "page_order": page_order, "hidden": hidden, "out_weight": out_weight, "norm_gain": norm_gain, "sectioned": sectioned, "routes": routes}


norm_epsilon = 1e-06

def attend(queries, new_kv, kv_pool, counts, fill, order):
    slot_count, pool_pages, page_size, lane_width = kv_pool.shape
    head_dim = lane_width // 2
    requests = queries.shape[0]
    score_scale = 1.0 / head_dim ** 0.5
    position = jnp.arange(pool_pages, dtype=jnp.int32)
    order = order.astype(jnp.int32)
    counts = counts.astype(jnp.int32)
    position_in_order = lax.optimization_barrier(jnp.sum(jnp.where(order[None, :] == position[:, None], position[None, :], 0), axis=1)).astype(jnp.int32)
    count_ends = jnp.cumsum(counts).astype(jnp.int32)
    starts = count_ends - counts
    owner_index = lax.optimization_barrier(jnp.sum((count_ends[None, :] <= position_in_order[:, None]).astype(jnp.int32), axis=1))
    member = owner_index[:, None] == jnp.arange(requests, dtype=jnp.int32)[None, :]
    member_float = member.astype(jnp.float32)
    within = position_in_order - lax.optimization_barrier(jnp.sum(jnp.where(member, starts[None, :], 0), axis=1))
    context = (counts - 1) * page_size + fill.astype(jnp.int32)
    context_limit = lax.optimization_barrier(jnp.sum(jnp.where(member, context[None, :], 0), axis=1))
    live_tokens = within[:, None] * page_size + jnp.arange(page_size, dtype=jnp.int32)[None, :] < context_limit[:, None]
    query_float = queries.astype(jnp.float32)
    page_queries = jnp.einsum('pr,rlgd->lpgd', member_float, query_float, precision=lax.Precision.HIGHEST)
    key_rows = kv_pool[..., :head_dim].astype(jnp.float32)
    value_rows = kv_pool[..., head_dim:].astype(jnp.float32)
    scores = jnp.einsum('lpgd,lptd->lpgt', page_queries, key_rows, precision=lax.Precision.HIGHEST) * score_scale
    scores = jnp.where(live_tokens[None, :, None, :], scores, -1e+30)
    page_top = lax.optimization_barrier(jnp.max(scores, axis=3))
    new_keys = new_kv[..., :head_dim].astype(jnp.float32)
    new_values = new_kv[..., head_dim:].astype(jnp.float32)
    fresh_score = jnp.einsum('rlgd,lrd->lrg', query_float, new_keys, precision=lax.Precision.HIGHEST) * score_scale
    masked_top = jnp.where(member.T[None, :, :, None], page_top[:, None, :, :], -1e+30)
    request_top = jnp.maximum(fresh_score, lax.optimization_barrier(jnp.max(masked_top, axis=2)))
    page_ref = jnp.einsum('pr,lrg->lpg', member_float, request_top, precision=lax.Precision.HIGHEST)
    weight = jnp.where(live_tokens[None, :, None, :], jnp.exp(scores - page_ref[..., None]), 0.0)
    page_den = lax.optimization_barrier(jnp.sum(weight, axis=3))
    weight_rounded = lax.optimization_barrier(weight.astype(jnp.bfloat16)).astype(jnp.float32)
    page_num = jnp.einsum('lpgt,lptd->lpgd', weight_rounded, value_rows, precision=lax.Precision.HIGHEST)
    fresh_weight = jnp.exp(fresh_score - request_top)
    fresh_rounded = lax.optimization_barrier(fresh_weight.astype(jnp.bfloat16)).astype(jnp.float32)
    denominator = jnp.einsum('pr,lpg->lrg', member_float, page_den, precision=lax.Precision.HIGHEST) + fresh_weight
    numerator = jnp.einsum('pr,lpgd->lrgd', member_float, page_num, precision=lax.Precision.HIGHEST)
    numerator = numerator + fresh_rounded[..., None] * new_values[:, :, None, :]
    attended = numerator / denominator[..., None]
    attended = jnp.transpose(attended, (1, 0, 2, 3)).astype(jnp.bfloat16)
    return attended.reshape(requests, -1)

def landing_table(destination, head_total, most_pages):
    sectioned_count = destination.shape[0]
    order_ids = jnp.arange(sectioned_count, dtype=jnp.int32)
    same_head = destination[:, None] == destination[None, :]
    earlier = order_ids[:, None] > order_ids[None, :]
    page_rank = lax.optimization_barrier(jnp.sum((same_head & earlier).astype(jnp.int32), axis=1))
    matches = (destination[None, None, :] == jnp.arange(head_total, dtype=jnp.int32)[:, None, None]) & (page_rank[None, None, :] == jnp.arange(most_pages, dtype=jnp.int32)[None, :, None])
    source_index = lax.optimization_barrier(jnp.sum(jnp.where(matches, order_ids[None, None, :], 0), axis=2)).astype(jnp.int32)
    source_valid = jnp.any(matches, axis=2)
    return (source_index, source_valid)

def reference(queries, new_kv, kv_pool, page_counts, last_fill, page_order, hidden, out_weight, norm_gain, sectioned, routes):
    group_size = Q_HEADS // CACHE_SLOTS
    pieces = []
    for owner_index in range(N_BATCH):
        first_row = owner_index * REQ_DEV
        query_block = queries[first_row:first_row + REQ_DEV].reshape(REQ_DEV, CACHE_SLOTS, group_size, HEAD_DIM)
        pool_block = kv_pool[:, owner_index * POOL_DEV:(owner_index + 1) * POOL_DEV]
        pieces.append(attend(query_block, new_kv[:, first_row:first_row + REQ_DEV], pool_block, page_counts[owner_index], last_fill[owner_index], page_order[owner_index]))
    attn = jnp.concatenate(pieces, axis=0)
    mixed = hidden.astype(jnp.float32) + jnp.dot(attn, out_weight, preferred_element_type=jnp.float32)
    residual_out = mixed.astype(jnp.bfloat16)
    mean_square = lax.optimization_barrier(jnp.mean(mixed * mixed, axis=1, keepdims=True))
    normed = (mixed * lax.rsqrt(mean_square + norm_epsilon) * norm_gain.astype(jnp.float32)).astype(jnp.bfloat16)
    table_fn = jax.vmap(jax.vmap(lambda destination: landing_table(destination, KV_HEADS, PER_HEAD_CAP)))
    source_index, source_valid = table_fn(routes[..., 0].astype(jnp.int32))
    slot_head = jnp.arange(CACHE_SLOTS, dtype=jnp.int32) * KV_HEADS // CACHE_SLOTS
    head_ids = jnp.arange(N_HEADS, dtype=jnp.int32)[None, None, :, None]
    batch_ids = jnp.arange(N_BATCH, dtype=jnp.int32)[None, :, None, None]
    slot_ids = slot_head[:, None, None, None]
    rank_ids = jnp.arange(PER_HEAD_CAP, dtype=jnp.int32)[None, None, None, :]
    chosen = source_index[head_ids, batch_ids, slot_ids, rank_ids]
    present = source_valid[head_ids, batch_ids, slot_ids, rank_ids]
    landed = sectioned[head_ids, batch_ids, chosen]
    arrival = jnp.where(present[..., None, None], landed, jnp.zeros_like(landed)).astype(jnp.bfloat16)
    return (residual_out, normed, arrival)
```

```python
import functools

import jax
import jax.numpy as jnp
from jax import lax
from jax.experimental import pallas as pl
from jax.experimental.pallas import tpu as pltpu
from jax.sharding import PartitionSpec as P

KV_HEADS = 8
PER_HEAD_CAP = 2
CORES = 2
CHUNK_PAGES = 8
norm_epsilon = 1e-06

MESH = pl.DeviceIdType.MESH
F32 = jnp.float32
BF16 = jnp.bfloat16


def page_limits(counts_ref, fill_ref, order_ref, page_size):
    requests, pool = counts_ref.shape[1], order_ref.shape[1]
    lane = lax.broadcasted_iota(jnp.int32, (requests, requests), 1)
    row = lax.broadcasted_iota(jnp.int32, (requests, requests), 0)
    counts = jnp.broadcast_to(counts_ref[...].astype(F32), (requests, requests))
    fill = jnp.broadcast_to(fill_ref[...].astype(F32), (requests, requests))
    count_col = jnp.sum(jnp.where(lane == row, counts, 0.0), axis=1, keepdims=True)
    fill_col = jnp.sum(jnp.where(lane == row, fill, 0.0), axis=1, keepdims=True)
    ends = jnp.sum(jnp.where(lane <= row, counts, 0.0), axis=1, keepdims=True)
    starts = ends - count_col
    context = (count_col - 1.0) * page_size + fill_col
    place = lax.broadcasted_iota(jnp.int32, (requests, 128), 1).astype(F32)
    live = jnp.clip(context - page_size * (place - starts), 0.0, float(page_size))
    live = jnp.where((place >= starts) & (place < ends), live, 0.0)
    order = jnp.broadcast_to(order_ref[...], (pool, pool))
    lane = lax.broadcasted_iota(jnp.int32, (pool, pool), 1)
    row = lax.broadcasted_iota(jnp.int32, (pool, pool), 0)
    order_col = jnp.sum(jnp.where(lane == row, order.astype(F32), 0.0), axis=1, keepdims=True)
    page = lax.broadcasted_iota(jnp.int32, (pool, 128), 1).astype(F32)
    one_hot = jnp.where(order_col == page, 1.0, 0.0).astype(BF16)
    return jnp.dot(live[:, :pool].astype(BF16), one_hot, preferred_element_type=F32)


def attend(q_ref, new_ref, kv, scores, limits):
    pool, page_size, width = kv.shape
    head_dim = width // 2
    requests = q_ref.shape[0]
    groups = q_ref.shape[1] // head_dim
    scale = 1.0 / head_dim**0.5
    q = jnp.concatenate([q_ref[:, g * head_dim : (g + 1) * head_dim] for g in range(groups)], axis=0)
    limits = jnp.concatenate([limits] * groups, axis=0)
    rows = groups * requests
    new_key = new_ref[:, :head_dim].astype(F32)
    new_value = new_ref[:, head_dim:].astype(F32)
    new_key = jnp.concatenate([new_key] * groups, axis=0)
    new_value = jnp.concatenate([new_value] * groups, axis=0)
    fresh = jnp.sum(q.astype(F32) * new_key, axis=1, keepdims=True) * scale
    token = lax.broadcasted_iota(jnp.int32, (rows, page_size), 1).astype(F32)
    top = jnp.full((rows, page_size), -1e30, F32)
    for first in range(0, pool, CHUNK_PAGES):
        keys = kv[first : first + CHUNK_PAGES, :, :head_dim].reshape(CHUNK_PAGES * page_size, head_dim)
        s = lax.dot_general(q, keys, (((1,), (1,)), ((), ())), preferred_element_type=F32) * scale
        for i in range(CHUNK_PAGES):
            part = s[:, i * page_size : (i + 1) * page_size]
            part = jnp.where(token < limits[:, first + i : first + i + 1], part, -1e30)
            top = jnp.maximum(top, part)
            scores[:, (first + i) * page_size : (first + i + 1) * page_size] = part
    top = jnp.maximum(jnp.max(top, axis=1, keepdims=True), fresh)
    den = jnp.zeros((rows, page_size), F32)
    num = jnp.zeros((rows, head_dim), F32)
    for first in range(0, pool, CHUNK_PAGES):
        cols = slice(first * page_size, (first + CHUNK_PAGES) * page_size)
        w = jnp.exp(scores[:, cols] - top)
        for i in range(CHUNK_PAGES):
            den = den + w[:, i * page_size : (i + 1) * page_size]
        values = kv[first : first + CHUNK_PAGES, :, head_dim:].reshape(CHUNK_PAGES * page_size, head_dim)
        num = num + jnp.dot(w.astype(BF16), values, preferred_element_type=F32)
    fresh_w = jnp.exp(fresh - top)
    den = jnp.sum(den, axis=1, keepdims=True) + fresh_w
    num = num + fresh_w.astype(BF16).astype(F32) * new_value
    out = (num / den).astype(BF16)
    return jnp.concatenate([out[g * requests : (g + 1) * requests] for g in range(groups)], axis=1)


def pack_slots(routes, pages, slots):
    count = pages.shape[0]
    heads, cap = slots.shape[:2]
    dest = [routes[j] for j in range(count)]
    rank = []
    for j in range(count):
        r = jnp.int32(0)
        for i in range(j):
            r = r + (dest[i] == dest[j]).astype(jnp.int32)
        rank.append(r)
    key = [dest[j] * cap + rank[j] for j in range(count)]
    for h in range(heads):
        for k in range(cap):
            index, found = jnp.int32(0), jnp.int32(0)
            for j in range(count):
                hit = (key[j] == h * cap + k).astype(jnp.int32)
                index = index + hit * j
                found = found + hit
            page = pages[index]
            slots[h, k] = jnp.where(found > 0, page, jnp.zeros_like(page))


def kernel(
    chips,
    q_ref,
    new_ref,
    counts_ref,
    fill_ref,
    order_ref,
    gain_ref,
    routes_ref,
    kv_in,
    hidden_in,
    weight_in,
    pages_in,
    arr,
    residual_ref,
    normed_ref,
    kv,
    weight,
    hidden,
    pages,
    slots,
    scores,
    part,
    sibling_part,
    terms,
    got_terms,
    blocks,
    load_sem,
    own_sem,
    page_send,
    near_sem,
    far_send,
    far_sem,
    partner_sem,
    core_send,
    core_sem,
    part_send,
    part_sem,
    term_send,
    term_sem,
    block_send,
    block_sem,
    share_send,
    share_sem,
):
    pairs = chips // 2
    reach = pairs // 2
    block = blocks.shape[3]
    a = lax.axis_index("heads")
    z, c = a // CORES, a % CORES
    pair, parity = z // 2, z % 2
    partner_z = z + 1 - 2 * parity
    sibling = z * CORES + (1 - c)

    def lane(zt):
        return zt * CORES + c

    def remote(src, dst, send, recv, dev):
        return pltpu.make_async_remote_copy(
            src_ref=src, dst_ref=dst, send_sem=send, recv_sem=recv, device_id={"heads": dev}, device_id_type=MESH
        )

    barrier = pltpu.get_barrier_semaphore()
    pl.semaphore_signal(barrier, inc=1, device_id={"heads": sibling}, device_id_type=MESH)
    for i in range(1, chips):
        pl.semaphore_signal(barrier, inc=1, device_id={"heads": lane((z + i) % chips)}, device_id_type=MESH)

    own_column = pl.multiple_of((c * chips + z) * block, block)
    loads = [
        pltpu.make_async_copy(pages_in, pages, load_sem.at[0]),
        pltpu.make_async_copy(kv_in, kv, load_sem.at[1]),
        pltpu.make_async_copy(weight_in, weight, load_sem.at[2]),
        pltpu.make_async_copy(hidden_in.at[:, pl.ds(own_column, block)], hidden, load_sem.at[3]),
    ]
    for copy in loads:
        copy.start()
    loads[0].wait()
    pack_slots(routes_ref, pages, slots)
    pl.semaphore_wait(barrier, chips)

    started = []

    def go(copy):
        copy.start()
        started.append(copy)

    own = pltpu.make_async_copy(slots.at[pair], arr.at[a], own_sem)
    own.start()
    go(remote(slots.at[pair], arr.at[a], page_send.at[0], partner_sem, lane(partner_z)))

    def clockwise(k):
        h = (pair + k) % pairs
        go(remote(slots.at[h], arr.at[a], page_send.at[2 * k - 1], near_sem.at[(k - 1) * 2 + parity], lane(2 * h)))

    def counter(k):
        h = (pair + pairs - k) % pairs
        go(remote(slots.at[h], arr.at[a], page_send.at[2 * k], near_sem.at[(k - 1) * 2 + parity], lane(2 * h + 1)))

    def opposite():
        h = (pair + reach) % pairs
        go(
            remote(
                slots.at[h],
                arr.at[a],
                page_send.at[2 * reach - 1],
                near_sem.at[2 * (reach - 1)],
                lane(2 * h + 1 - parity),
            )
        )

    def source(m, side):
        if m == 2 * (reach - 1):
            zs = 2 * ((pair + reach) % pairs) + 1 - side
        else:
            k, sp = m // 2 + 1, m % 2
            zs = 2 * ((pair + pairs + (2 * side - 1) * k) % pairs) + sp
        return zs

    def to_sibling(zs):
        row = arr.at[lane(zs)]
        go(remote(row, row, core_send.at[zs], core_sem.at[zs], sibling))

    def relay_near(m):
        zs = source(m, parity)
        row = arr.at[lane(zs)]
        remote(row, row, far_send.at[m], near_sem.at[m], lane(partner_z)).wait_recv()
        go(remote(row, row, far_send.at[m], far_sem.at[m], lane(partner_z)))
        to_sibling(zs)

    def take_far(m):
        zs = source(m, 1 - parity)
        row = arr.at[lane(zs)]
        remote(row, row, far_send.at[m], far_sem.at[m], lane(partner_z)).wait_recv()
        to_sibling(zs)

    clockwise(1)
    counter(1)
    clockwise(2)
    counter(2)

    limits = page_limits(counts_ref, fill_ref, order_ref, kv.shape[1])
    loads[1].wait()
    attn = attend(q_ref, new_ref, kv, scores, limits)
    loads[2].wait()
    for half in range(CORES):

        def project(zz, _, half=half):
            columns = pl.ds(pl.multiple_of((half * chips + zz) * block, block), block)
            part[half, zz] = jnp.dot(attn, weight[:, columns], preferred_element_type=F32)
            return 0

        lax.fori_loop(0, chips, project, 0, unroll=4)

    own.wait()
    to_sibling(z)
    exchange = remote(part.at[1 - c], sibling_part, part_send, part_sem, sibling)
    exchange.start()
    exchange.wait_recv()

    def add_cores(zz, _):
        terms[zz] = (part[c, zz] + sibling_part[zz]).astype(BF16)
        return 0

    lax.fori_loop(0, chips, add_cores, 0, unroll=4)
    total = part[c, z] + sibling_part[z]
    for i in range(1, chips):
        zt = (z + i) % chips
        go(remote(terms.at[zt], got_terms.at[i - 1], term_send.at[i - 1], term_sem.at[i - 1], lane(zt)))
    clockwise(3)
    counter(3)
    relay_near(0)
    relay_near(1)
    remote(arr.at[lane(partner_z)], arr.at[lane(partner_z)], page_send.at[0], partner_sem, sibling).wait_recv()
    to_sibling(partner_z)

    for i in range(1, chips):
        remote(terms.at[0], got_terms.at[i - 1], term_send.at[i - 1], term_sem.at[i - 1], sibling).wait_recv()
        total = total + got_terms[i - 1].astype(F32)
    loads[3].wait()
    blocks[c, z] = (hidden[...].astype(F32) + total).astype(BF16)
    relay_near(2)
    relay_near(3)
    mine = blocks.at[c, z]
    for i in range(1, chips):
        go(remote(mine, mine, block_send.at[i - 1], block_sem.at[i - 1], lane((z + i) % chips)))
    opposite()
    take_far(0)
    take_far(1)
    take_far(2)
    take_far(3)
    for i in range(1, chips):
        theirs = blocks.at[c, (z + chips - i) % chips]
        remote(theirs, theirs, block_send.at[i - 1], block_sem.at[i - 1], sibling).wait_recv()
    share = remote(blocks.at[c], blocks.at[c], share_send, share_sem, sibling)
    share.start()
    relay_near(4)
    relay_near(5)
    remote(blocks.at[1 - c], blocks.at[1 - c], share_send, share_sem, sibling).wait_recv()

    def squares(b, acc):
        x = blocks[b // chips, b % chips].astype(F32)
        return acc + x * x

    width = CORES * chips * block
    acc = lax.fori_loop(0, CORES * chips, squares, jnp.zeros(blocks.shape[2:], F32), unroll=4)
    inverse = lax.rsqrt(jnp.sum(acc, axis=1, keepdims=True) / width + norm_epsilon)

    def finish(b, _):
        columns = pl.ds(pl.multiple_of(b * block, block), block)
        x = blocks[b // chips, b % chips]
        residual_ref[:, columns] = x
        normed_ref[:, columns] = (x.astype(F32) * inverse * gain_ref[:, columns].astype(F32)).astype(BF16)
        return 0

    lax.fori_loop(0, CORES * chips, finish, 0, unroll=4)

    relay_near(6)
    take_far(4)
    take_far(5)
    take_far(6)
    for i in range(chips):
        theirs = arr.at[i * CORES + 1 - c]
        remote(theirs, theirs, core_send.at[i], core_sem.at[i], sibling).wait_recv()
    exchange.wait_send()
    share.wait_send()
    for copy in started:
        copy.wait_send()


def per_device(
    queries,
    new_kv,
    kv_pool,
    page_counts,
    last_fill,
    page_order,
    hidden,
    out_weight,
    norm_gain,
    sectioned,
    routes,
):
    head_count = lax.axis_size("heads")
    chips = head_count // CORES
    requests, width = hidden.shape
    _, pool, page_size, kv_width = kv_pool.shape
    page_count = sectioned.shape[2]
    block = width // head_count
    pairs = chips // 2
    near = pairs - 1
    if pairs != KV_HEADS or new_kv.shape[0] != 1:
        raise ValueError("unexpected layout")
    vmem = pl.BlockSpec(memory_space=pltpu.VMEM)
    smem = pl.BlockSpec(memory_space=pltpu.SMEM)
    anywhere = pl.BlockSpec(memory_space=pl.ANY)
    dma = pltpu.SemaphoreType.DMA
    slot_shape = (PER_HEAD_CAP, page_size, kv_width)
    arrival, residual, normed = pl.pallas_call(
        functools.partial(kernel, chips),
        out_shape=(
            jax.ShapeDtypeStruct((head_count, *slot_shape), BF16),
            jax.ShapeDtypeStruct((requests, width), BF16),
            jax.ShapeDtypeStruct((requests, width), BF16),
        ),
        in_specs=[vmem] * 6 + [smem] + [anywhere] * 4,
        out_specs=(anywhere, vmem, vmem),
        scratch_shapes=[
            pltpu.VMEM((pool, page_size, kv_width), BF16),
            pltpu.VMEM(out_weight.shape, BF16),
            pltpu.VMEM((requests, block), BF16),
            pltpu.VMEM((page_count, page_size, kv_width), BF16),
            pltpu.VMEM((KV_HEADS, *slot_shape), BF16),
            pltpu.VMEM((requests * queries.shape[1] * 2 // kv_width, pool * page_size), F32),
            pltpu.VMEM((CORES, chips, requests, block), F32),
            pltpu.VMEM((chips, requests, block), F32),
            pltpu.VMEM((chips, requests, block), BF16),
            pltpu.VMEM((chips - 1, requests, block), BF16),
            pltpu.VMEM((CORES, chips, requests, block), BF16),
            dma((4,)),
            dma,
            dma((pairs,)),
            dma((near,)),
            dma((near,)),
            dma((near,)),
            dma,
            dma((chips,)),
            dma((chips,)),
            dma,
            dma,
            dma((chips - 1,)),
            dma((chips - 1,)),
            dma((chips - 1,)),
            dma((chips - 1,)),
            dma,
            dma,
        ],
        compiler_params=pltpu.CompilerParams(
            collective_id=0, has_side_effects=True, vmem_limit_bytes=40 * 1024 * 1024
        ),
    )(
        queries,
        new_kv[0],
        page_counts,
        last_fill,
        page_order,
        norm_gain.reshape(1, width),
        routes.reshape(page_count),
        kv_pool[0],
        hidden,
        out_weight,
        sectioned[0, 0],
    )
    return (residual, normed, arrival[None, None])


def solution(mesh):
    return jax.shard_map(
        per_device,
        mesh=mesh,
        in_specs=(
            P(("groups", "batch"), "heads"),
            P(("groups", "heads"), "batch", None),
            P(("groups", "heads"), "batch", None, None),
            P(("groups", "batch"), None),
            P(("groups", "batch"), None),
            P(("groups", "batch"), None),
            P(("groups", "batch"), None),
            P("heads", None),
            P(),
            P(("groups", "heads"), "batch", None, None, None),
            P(("groups", "heads"), "batch", None, None),
        ),
        out_specs=(
            P(("groups", "batch"), None),
            P(("groups", "batch"), None),
            P(("groups", "heads"), "batch", None, None, None, None),
        ),
        check_vma=False,
    )
```

```python
import functools

import jax
import jax.numpy as jnp
from jax import lax
from jax.experimental import pallas as pl
from jax.experimental.pallas import tpu as pltpu
from jax.sharding import PartitionSpec as P

KV_HEADS = 8
PER_HEAD_CAP = 2
CORES = 2
CHUNK_PAGES = 8
LANES = 128
PLAN = (
    "cw1",
    "ccw1",
    "tell2",
    "scores",
    "know2",
    "cw2",
    "ccw2",
    "tell4",
    "attention",
    "know4",
    "terms",
    "relay0",
    "relay1",
    "partner",
    "pair",
    "cw3",
    "ccw3",
    "relay2",
    "relay3",
    "sum",
    "block",
    "opposite",
    "far0",
    "far1",
    "far2",
    "far3",
    "relay4",
    "relay5",
    "brelay",
    "relay6",
    "share",
    "norm",
    "far4",
    "far5",
    "far6",
)
norm_epsilon = 1e-06

MESH = pl.DeviceIdType.MESH
F32 = jnp.float32
BF16 = jnp.bfloat16


def page_limits(counts_ref, fill_ref, order_ref, page_size):
    requests, pool = counts_ref.shape[1], order_ref.shape[1]
    lane = lax.broadcasted_iota(jnp.int32, (requests, requests), 1)
    row = lax.broadcasted_iota(jnp.int32, (requests, requests), 0)
    counts = jnp.broadcast_to(counts_ref[...].astype(F32), (requests, requests))
    fill = jnp.broadcast_to(fill_ref[...].astype(F32), (requests, requests))
    count_col = jnp.sum(jnp.where(lane == row, counts, 0.0), axis=1, keepdims=True)
    fill_col = jnp.sum(jnp.where(lane == row, fill, 0.0), axis=1, keepdims=True)
    ends = jnp.sum(jnp.where(lane <= row, counts, 0.0), axis=1, keepdims=True)
    starts = ends - count_col
    context = (count_col - 1.0) * page_size + fill_col
    place = lax.broadcasted_iota(jnp.int32, (requests, 128), 1).astype(F32)
    live = jnp.clip(context - page_size * (place - starts), 0.0, float(page_size))
    live = jnp.where((place >= starts) & (place < ends), live, 0.0)
    order = jnp.broadcast_to(order_ref[...], (pool, pool))
    lane = lax.broadcasted_iota(jnp.int32, (pool, pool), 1)
    row = lax.broadcasted_iota(jnp.int32, (pool, pool), 0)
    order_col = jnp.sum(jnp.where(lane == row, order.astype(F32), 0.0), axis=1, keepdims=True)
    page = lax.broadcasted_iota(jnp.int32, (pool, 128), 1).astype(F32)
    one_hot = jnp.where(order_col == page, 1.0, 0.0).astype(BF16)
    return jnp.dot(live[:, :pool].astype(BF16), one_hot, preferred_element_type=F32)


def attend_scores(q_ref, new_ref, kv, scores, limits):
    pool, page_size, width = kv.shape
    head_dim = width // 2
    requests = q_ref.shape[0]
    groups = q_ref.shape[1] // head_dim
    scale = 1.0 / head_dim**0.5
    q = jnp.concatenate([q_ref[:, g * head_dim : (g + 1) * head_dim] for g in range(groups)], axis=0)
    limits = jnp.concatenate([limits] * groups, axis=0)
    rows = groups * requests
    new_key = jnp.concatenate([new_ref[:, :head_dim].astype(F32)] * groups, axis=0)
    fresh = jnp.sum(q.astype(F32) * new_key, axis=1, keepdims=True) * scale
    token = lax.broadcasted_iota(jnp.int32, (rows, page_size), 1).astype(F32)
    top = jnp.full((rows, page_size), -1e30, F32)
    for first in range(0, pool, CHUNK_PAGES):
        keys = kv[first : first + CHUNK_PAGES, :, :head_dim].reshape(CHUNK_PAGES * page_size, head_dim)
        s = lax.dot_general(q, keys, (((1,), (1,)), ((), ())), preferred_element_type=F32) * scale
        for i in range(CHUNK_PAGES):
            part = s[:, i * page_size : (i + 1) * page_size]
            part = jnp.where(token < limits[:, first + i : first + i + 1], part, -1e30)
            top = jnp.maximum(top, part)
            scores[:, (first + i) * page_size : (first + i + 1) * page_size] = part
    return jnp.maximum(jnp.max(top, axis=1, keepdims=True), fresh), fresh


def attend_values(q_ref, new_ref, kv, scores, top, fresh):
    pool, page_size, width = kv.shape
    head_dim = width // 2
    requests = q_ref.shape[0]
    groups = q_ref.shape[1] // head_dim
    rows = groups * requests
    new_value = jnp.concatenate([new_ref[:, head_dim:].astype(F32)] * groups, axis=0)
    den = jnp.zeros((rows, page_size), F32)
    num = jnp.zeros((rows, head_dim), F32)
    for first in range(0, pool, CHUNK_PAGES):
        cols = slice(first * page_size, (first + CHUNK_PAGES) * page_size)
        w = jnp.exp(scores[:, cols] - top)
        for i in range(CHUNK_PAGES):
            den = den + w[:, i * page_size : (i + 1) * page_size]
        values = kv[first : first + CHUNK_PAGES, :, head_dim:].reshape(CHUNK_PAGES * page_size, head_dim)
        num = num + jnp.dot(w.astype(BF16), values, preferred_element_type=F32)
    fresh_w = jnp.exp(fresh - top)
    den = jnp.sum(den, axis=1, keepdims=True) + fresh_w
    num = num + fresh_w.astype(BF16).astype(F32) * new_value
    out = (num / den).astype(BF16)
    return jnp.concatenate([out[g * requests : (g + 1) * requests] for g in range(groups)], axis=1)


def pack_slots(routes, pages, slots):
    count = pages.shape[0]
    heads, cap = slots.shape[:2]
    dest = [routes[j] for j in range(count)]
    rank = []
    for j in range(count):
        r = jnp.int32(0)
        for i in range(j):
            r = r + (dest[i] == dest[j]).astype(jnp.int32)
        rank.append(r)
    key = [dest[j] * cap + rank[j] for j in range(count)]
    for h in range(heads):
        for k in range(cap):
            index, found = jnp.int32(0), jnp.int32(0)
            for j in range(count):
                hit = (key[j] == h * cap + k).astype(jnp.int32)
                index = index + hit * j
                found = found + hit
            page = pages[index]
            slots[h, k] = jnp.where(found > 0, page, jnp.zeros_like(page))


def kernel(
    chips,
    q_in,
    new_in,
    counts_in,
    fill_in,
    order_in,
    gain_in,
    routes_in,
    kv_in,
    hidden_in,
    weight_in,
    pages_in,
    arr,
    residual_ref,
    normed_ref,
    q_ref,
    new_ref,
    counts_ref,
    fill_ref,
    order_ref,
    gain_ref,
    routes_ref,
    kv,
    weight,
    hidden,
    pages,
    slots,
    gain_wide,
    scores,
    part,
    sibling_part,
    give,
    got_pair,
    terms,
    got_terms,
    blocks,
    load_sem,
    own_sem,
    page_send,
    near_sem,
    far_send,
    far_sem,
    partner_sem,
    core_send,
    core_sem,
    part_send,
    part_sem,
    pair_send,
    pair_sem,
    term_send,
    term_sem,
    block_send,
    block_near,
    block_relay,
    block_far,
    block_partner,
    share_send,
    share_sem,
    wave_two,
    wave_four,
):
    pairs = chips // 2
    reach = pairs // 2
    block = blocks.shape[3]
    a = lax.axis_index("heads")
    z, c = a // CORES, a % CORES
    pair, parity = z // 2, z % 2
    partner_z = z + 1 - 2 * parity
    sibling = z * CORES + (1 - c)

    def lane(zt):
        return zt * CORES + c

    def remote(src, dst, send, recv, dev):
        return pltpu.make_async_remote_copy(
            src_ref=src, dst_ref=dst, send_sem=send, recv_sem=recv, device_id={"heads": dev}, device_id_type=MESH
        )

    def chip_of(k, side):
        return 2 * ((pair + pairs + k) % pairs) + side

    def signal(sem, dev):
        pl.semaphore_signal(sem, inc=1, device_id={"heads": dev}, device_id_type=MESH)

    barrier = pltpu.get_barrier_semaphore()
    signal(barrier, sibling)
    signal(barrier, lane(partner_z))
    for k in (-1, 1):
        for side in (0, 1):
            signal(barrier, lane(chip_of(k, side)))

    own_column = pl.multiple_of((c * chips + z) * block, block)
    loads = {
        name: pltpu.make_async_copy(src, dst, load_sem.at[i])
        for i, (name, src, dst) in enumerate(
            (
                ("routes", routes_in, routes_ref),
                ("pages", pages_in, pages),
                ("q", q_in, q_ref),
                ("new", new_in, new_ref),
                ("counts", counts_in, counts_ref),
                ("fill", fill_in, fill_ref),
                ("order", order_in, order_ref),
                ("kv", kv_in, kv),
                ("weight", weight_in, weight),
                ("hidden", hidden_in.at[:, pl.ds(own_column, block)], hidden),
                ("gain", gain_in, gain_ref),
            )
        )
    }
    for copy in loads.values():
        copy.start()
    loads["routes"].wait()
    loads["pages"].wait()
    pack_slots(routes_ref, pages, slots)
    pl.semaphore_wait(barrier, 6)

    def wave(sem, k):
        signal(sem, lane(chip_of(k, parity)))
        signal(sem, lane(chip_of(-k, parity)))


    started = []

    def go(copy):
        copy.start()
        started.append(copy)

    own = pltpu.make_async_copy(slots.at[pair], arr.at[a], own_sem)
    own.start()
    go(remote(slots.at[pair], arr.at[a], page_send.at[0], partner_sem, lane(partner_z)))

    def clockwise(k):
        h = (pair + k) % pairs
        go(remote(slots.at[h], arr.at[a], page_send.at[2 * k - 1], near_sem.at[(k - 1) * 2 + parity], lane(2 * h)))

    def counter(k):
        h = (pair + pairs - k) % pairs
        go(remote(slots.at[h], arr.at[a], page_send.at[2 * k], near_sem.at[(k - 1) * 2 + parity], lane(2 * h + 1)))

    def opposite():
        h = (pair + reach) % pairs
        go(
            remote(
                slots.at[h],
                arr.at[a],
                page_send.at[2 * reach - 1],
                near_sem.at[2 * (reach - 1)],
                lane(2 * h + 1 - parity),
            )
        )

    def source(m, side):
        if m == 2 * (reach - 1):
            zs = 2 * ((pair + reach) % pairs) + 1 - side
        else:
            k, sp = m // 2 + 1, m % 2
            zs = 2 * ((pair + pairs + (2 * side - 1) * k) % pairs) + sp
        return zs

    def to_sibling(zs):
        row = arr.at[lane(zs)]
        go(remote(row, row, core_send.at[zs], core_sem.at[zs], sibling))

    def relay_near(m):
        zs = source(m, parity)
        row = arr.at[lane(zs)]
        remote(row, row, far_send.at[m], near_sem.at[m], lane(partner_z)).wait_recv()
        go(remote(row, row, far_send.at[m], far_sem.at[m], lane(partner_z)))
        to_sibling(zs)

    def take_far(m):
        zs = source(m, 1 - parity)
        row = arr.at[lane(zs)]
        remote(row, row, far_send.at[m], far_sem.at[m], lane(partner_z)).wait_recv()
        to_sibling(zs)

    exchange = remote(part.at[1 - c], sibling_part, part_send, part_sem, sibling)
    share = remote(blocks.at[c], blocks.at[c], share_send, share_sem, sibling)

    state = {}

    def attention_scores():
        for name in ("q", "new", "counts", "fill", "order"):
            loads[name].wait()
        limits = page_limits(counts_ref, fill_ref, order_ref, kv.shape[1])
        loads["kv"].wait()
        state["top"], state["fresh"] = attend_scores(q_ref, new_ref, kv, scores, limits)

    def attention():
        attn = attend_values(q_ref, new_ref, kv, scores, state["top"], state["fresh"])
        loads["weight"].wait()
        for half in range(CORES):

            def project(zz, _, half=half):
                columns = pl.ds(pl.multiple_of((half * chips + zz) * block, block), block)
                part[half, zz] = jnp.dot(attn, weight[:, columns], preferred_element_type=F32)
                return 0

            lax.fori_loop(0, chips, project, 0, unroll=4)
        own.wait()
        to_sibling(z)
        exchange.start()

    near = 2 * reach - 1

    def owner(m, side):
        if m == near - 1:
            return 2 * ((pair + reach) % pairs) + 1 - side
        return 2 * ((pair + pairs + (2 * side - 1) * (m // 2 + 1)) % pairs) + m % 2

    def core_sum(zt):
        return part[c, zt] + sibling_part[zt]

    pair_exchange = remote(give, got_pair, pair_send, pair_sem, lane(partner_z))

    def send_terms():
        exchange.wait_recv()
        for m in range(near):
            give[m] = core_sum(owner(m, 1 - parity)).astype(BF16)
        give[near] = core_sum(partner_z).astype(BF16)
        pair_exchange.start()

    def send_pair_terms():
        pair_exchange.wait_recv()
        for m in range(near):
            terms[m] = (core_sum(owner(m, parity)) + got_pair[m].astype(F32)).astype(BF16)
        for m in range(near):
            place = near - 1 if m == near - 1 else (1 - parity) * (reach - 1) + m // 2
            to = lane(owner(m, parity))
            go(remote(terms.at[m], got_terms.at[place], term_send.at[m], term_sem.at[place], to))

    def sum_terms():
        total = core_sum(z) + got_pair[near].astype(F32)
        for m in range(near):
            remote(terms.at[m], got_terms.at[m], term_send.at[m], term_sem.at[m], sibling).wait_recv()
            total = total + got_terms[m].astype(F32)
        loads["hidden"].wait()
        blocks[c, z] = (hidden[...].astype(F32) + total).astype(BF16)

    def send_block():
        mine = blocks.at[c, z]
        go(remote(mine, mine, block_send.at[near], block_partner, lane(partner_z)))
        for m in range(near):
            k = m // 2 + 1
            if m == near - 1:
                at, zt = near - 1, 2 * ((pair + reach) % pairs) + 1 - parity
            elif m % 2 == 0:
                at, zt = (k - 1) * 2 + parity, 2 * ((pair + k) % pairs)
            else:
                at, zt = (k - 1) * 2 + parity, 2 * ((pair + pairs - k) % pairs) + 1
            go(remote(mine, mine, block_send.at[m], block_near.at[at], lane(zt)))

    def relay_blocks():
        for m in range(near):
            theirs = blocks.at[c, source(m, parity)]
            remote(theirs, theirs, block_relay.at[m], block_near.at[m], sibling).wait_recv()
            go(remote(theirs, theirs, block_relay.at[m], block_far.at[m], lane(partner_z)))

    def share_blocks():
        theirs = blocks.at[c, partner_z]
        remote(theirs, theirs, block_send.at[near], block_partner, sibling).wait_recv()
        for m in range(near):
            theirs = blocks.at[c, source(m, 1 - parity)]
            remote(theirs, theirs, block_relay.at[m], block_far.at[m], sibling).wait_recv()
        share.start()

    def norm():
        remote(blocks.at[1 - c], blocks.at[1 - c], share_send, share_sem, sibling).wait_recv()

        def squares(b, acc):
            x = blocks[b // chips, b % chips].astype(F32)
            return acc + x * x

        width = CORES * chips * block
        acc = lax.fori_loop(0, CORES * chips, squares, jnp.zeros(blocks.shape[2:], F32), unroll=4)
        inverse = lax.rsqrt(jnp.sum(acc, axis=1, keepdims=True) / width + norm_epsilon)
        loads["gain"].wait()
        gain_wide[...] = gain_ref[...].astype(F32)
        lanes = gain_wide.shape[1]
        rows = block // lanes

        def finish(b, _):
            columns = pl.ds(pl.multiple_of(b * block, block), block)
            x = blocks[b // chips, b % chips]
            gain = jnp.concatenate([gain_wide[pl.ds(b * rows + i, 1), :] for i in range(rows)], axis=1)
            residual_ref[:, columns] = x
            normed_ref[:, columns] = (x.astype(F32) * inverse * gain).astype(BF16)
            return 0

        lax.fori_loop(0, CORES * chips, finish, 0, unroll=4)

    def take_partner():
        row = arr.at[lane(partner_z)]
        remote(row, row, page_send.at[0], partner_sem, sibling).wait_recv()
        to_sibling(partner_z)

    named = {
        "scores": attention_scores,
        "attention": attention,
        "tell2": lambda: wave(wave_two, 1),
        "know2": lambda: pl.semaphore_wait(wave_two, 2),
        "tell4": lambda: wave(wave_four, 2),
        "know4": lambda: pl.semaphore_wait(wave_four, 2),
        "terms": send_terms,
        "pair": send_pair_terms,
        "brelay": relay_blocks,
        "sum": sum_terms,
        "block": send_block,
        "share": share_blocks,
        "norm": norm,
        "partner": take_partner,
        "opposite": opposite,
    }
    numbered = {"cw": clockwise, "ccw": counter, "relay": relay_near, "far": take_far}
    for step in PLAN:
        if step in named:
            named[step]()
        else:
            word = step.rstrip("0123456789")
            numbered[word](int(step[len(word) :]))

    for i in range(chips):
        theirs = arr.at[i * CORES + 1 - c]
        remote(theirs, theirs, core_send.at[i], core_sem.at[i], sibling).wait_recv()
    exchange.wait_send()
    pair_exchange.wait_send()
    share.wait_send()
    for copy in started:
        copy.wait_send()


def per_device(
    queries,
    new_kv,
    kv_pool,
    page_counts,
    last_fill,
    page_order,
    hidden,
    out_weight,
    norm_gain,
    sectioned,
    routes,
):
    head_count = lax.axis_size("heads")
    chips = head_count // CORES
    requests, width = hidden.shape
    _, pool, page_size, kv_width = kv_pool.shape
    page_count = sectioned.shape[2]
    block = width // head_count
    pairs = chips // 2
    near = pairs - 1
    if pairs != KV_HEADS or pairs != 8 or new_kv.shape[0] != 1:
        raise ValueError("unexpected layout")
    vmem = pl.BlockSpec(memory_space=pltpu.VMEM)
    hbm = pl.BlockSpec(memory_space=pltpu.HBM)
    anywhere = pl.BlockSpec(memory_space=pl.ANY)
    dma = pltpu.SemaphoreType.DMA
    slot_shape = (PER_HEAD_CAP, page_size, kv_width)
    arrival, residual, normed = pl.pallas_call(
        functools.partial(kernel, chips),
        out_shape=(
            pltpu.VMEM((head_count, *slot_shape), BF16),
            jax.ShapeDtypeStruct((requests, width), BF16),
            jax.ShapeDtypeStruct((requests, width), BF16),
        ),
        in_specs=[hbm] * 11,
        out_specs=(anywhere, vmem, vmem),
        scratch_shapes=[
            pltpu.VMEM(queries.shape, BF16),
            pltpu.VMEM(new_kv.shape[1:], BF16),
            pltpu.VMEM(page_counts.shape, jnp.int32),
            pltpu.VMEM(last_fill.shape, jnp.int32),
            pltpu.VMEM(page_order.shape, jnp.int32),
            pltpu.VMEM((width // LANES, LANES), BF16),
            pltpu.SMEM((page_count,), jnp.int32),
            pltpu.VMEM((pool, page_size, kv_width), BF16),
            pltpu.VMEM(out_weight.shape, BF16),
            pltpu.VMEM((requests, block), BF16),
            pltpu.VMEM((page_count, page_size, kv_width), BF16),
            pltpu.VMEM((KV_HEADS, *slot_shape), BF16),
            pltpu.VMEM((width // LANES, LANES), F32),
            pltpu.VMEM((requests * queries.shape[1] * 2 // kv_width, pool * page_size), F32),
            pltpu.VMEM((CORES, chips, requests, block), F32),
            pltpu.VMEM((chips, requests, block), F32),
            pltpu.VMEM((near + 1, requests, block), BF16),
            pltpu.VMEM((near + 1, requests, block), BF16),
            pltpu.VMEM((near, requests, block), BF16),
            pltpu.VMEM((near, requests, block), BF16),
            pltpu.VMEM((CORES, chips, requests, block), BF16),
            dma((11,)),
            dma,
            dma((pairs,)),
            dma((near,)),
            dma((near,)),
            dma((near,)),
            dma,
            dma((chips,)),
            dma((chips,)),
            dma,
            dma,
            dma,
            dma,
            dma((near,)),
            dma((near,)),
            dma((near + 1,)),
            dma((near,)),
            dma((near,)),
            dma((near,)),
            dma,
            dma,
            dma,
            pltpu.SemaphoreType.REGULAR,
            pltpu.SemaphoreType.REGULAR,
        ],
        compiler_params=pltpu.CompilerParams(
            collective_id=0, has_side_effects=True, vmem_limit_bytes=40 * 1024 * 1024
        ),
    )(*[pltpu.with_memory_space_constraint(x, pltpu.HBM) for x in (
        queries,
        new_kv[0],
        page_counts,
        last_fill,
        page_order,
        norm_gain.reshape(width // LANES, LANES),
        routes.reshape(page_count),
        kv_pool[0],
        hidden,
        out_weight,
        sectioned[0, 0],
    )])
    return (residual, normed, arrival[None, None])


def solution(mesh):
    return jax.shard_map(
        per_device,
        mesh=mesh,
        in_specs=(
            P(("groups", "batch"), "heads"),
            P(("groups", "heads"), "batch", None),
            P(("groups", "heads"), "batch", None, None),
            P(("groups", "batch"), None),
            P(("groups", "batch"), None),
            P(("groups", "batch"), None),
            P(("groups", "batch"), None),
            P("heads", None),
            P(),
            P(("groups", "heads"), "batch", None, None, None),
            P(("groups", "heads"), "batch", None, None),
        ),
        out_specs=(
            P(("groups", "batch"), None),
            P(("groups", "batch"), None),
            P(("groups", "heads"), "batch", None, None, None, None),
        ),
        check_vma=False,
    )
```

```python
import functools

import jax
import jax.numpy as jnp
from jax import lax
from jax.experimental import pallas as pl
from jax.experimental.pallas import tpu as pltpu
from jax.sharding import PartitionSpec as P

KV_HEADS = 8
PER_HEAD_CAP = 2
CORES = 2
CHUNK_PAGES = 8
LANES = 128
ARRIVAL_COPIES = 4
PLAN = (
    "toward1",
    "away1",
    "tell2",
    "scores",
    "know2",
    "away2",
    "toward2",
    "tell4",
    "attention",
    "know4",
    "terms",
    "away3",
    "relay0",
    "relay1",
    "partner",
    "pair",
    "toward3",
    "relay2",
    "relay3",
    "opposite",
    "sum",
    "block",
    "relay4",
    "relay5",
    "brelay",
    "relay6",
    "relay7",
    "far0",
    "far1",
    "far2",
    "far3",
    "share",
    "shared",
    "far4",
    "far5",
    "far6",
    "far7",
)
norm_epsilon = 1e-06

MESH = pl.DeviceIdType.MESH
F32 = jnp.float32
BF16 = jnp.bfloat16


def page_limits(counts_ref, fill_ref, order_ref, page_size):
    requests, pool = counts_ref.shape[1], order_ref.shape[1]
    lane = lax.broadcasted_iota(jnp.int32, (requests, requests), 1)
    row = lax.broadcasted_iota(jnp.int32, (requests, requests), 0)
    counts = jnp.broadcast_to(counts_ref[...].astype(F32), (requests, requests))
    fill = jnp.broadcast_to(fill_ref[...].astype(F32), (requests, requests))
    count_col = jnp.sum(jnp.where(lane == row, counts, 0.0), axis=1, keepdims=True)
    fill_col = jnp.sum(jnp.where(lane == row, fill, 0.0), axis=1, keepdims=True)
    ends = jnp.sum(jnp.where(lane <= row, counts, 0.0), axis=1, keepdims=True)
    starts = ends - count_col
    context = (count_col - 1.0) * page_size + fill_col
    place = lax.broadcasted_iota(jnp.int32, (requests, 128), 1).astype(F32)
    live = jnp.clip(context - page_size * (place - starts), 0.0, float(page_size))
    live = jnp.where((place >= starts) & (place < ends), live, 0.0)
    order = jnp.broadcast_to(order_ref[...], (pool, pool))
    lane = lax.broadcasted_iota(jnp.int32, (pool, pool), 1)
    row = lax.broadcasted_iota(jnp.int32, (pool, pool), 0)
    order_col = jnp.sum(jnp.where(lane == row, order.astype(F32), 0.0), axis=1, keepdims=True)
    page = lax.broadcasted_iota(jnp.int32, (pool, 128), 1).astype(F32)
    one_hot = jnp.where(order_col == page, 1.0, 0.0).astype(BF16)
    return jnp.dot(live[:, :pool].astype(BF16), one_hot, preferred_element_type=F32)


def attend_scores(q_ref, new_ref, kv, scores, limits):
    pool, page_size, width = kv.shape
    head_dim = width // 2
    requests = q_ref.shape[0]
    groups = q_ref.shape[1] // head_dim
    scale = 1.0 / head_dim**0.5
    q = jnp.concatenate([q_ref[:, g * head_dim : (g + 1) * head_dim] for g in range(groups)], axis=0)
    limits = jnp.concatenate([limits] * groups, axis=0)
    rows = groups * requests
    new_key = jnp.concatenate([new_ref[:, :head_dim].astype(F32)] * groups, axis=0)
    fresh = jnp.sum(q.astype(F32) * new_key, axis=1, keepdims=True) * scale
    token = lax.broadcasted_iota(jnp.int32, (rows, page_size), 1).astype(F32)
    top = jnp.full((rows, page_size), -1e30, F32)
    for first in range(0, pool, CHUNK_PAGES):
        keys = kv[first : first + CHUNK_PAGES, :, :head_dim].reshape(CHUNK_PAGES * page_size, head_dim)
        s = lax.dot_general(q, keys, (((1,), (1,)), ((), ())), preferred_element_type=F32) * scale
        for i in range(CHUNK_PAGES):
            part = s[:, i * page_size : (i + 1) * page_size]
            part = jnp.where(token < limits[:, first + i : first + i + 1], part, -1e30)
            top = jnp.maximum(top, part)
            scores[:, (first + i) * page_size : (first + i + 1) * page_size] = part
    return jnp.maximum(jnp.max(top, axis=1, keepdims=True), fresh), fresh


def attend_values(q_ref, new_ref, kv, scores, top, fresh):
    pool, page_size, width = kv.shape
    head_dim = width // 2
    requests = q_ref.shape[0]
    groups = q_ref.shape[1] // head_dim
    rows = groups * requests
    new_value = jnp.concatenate([new_ref[:, head_dim:].astype(F32)] * groups, axis=0)
    den = jnp.zeros((rows, page_size), F32)
    num = jnp.zeros((rows, head_dim), F32)
    for first in range(0, pool, CHUNK_PAGES):
        cols = slice(first * page_size, (first + CHUNK_PAGES) * page_size)
        w = jnp.exp(scores[:, cols] - top)
        for i in range(CHUNK_PAGES):
            den = den + w[:, i * page_size : (i + 1) * page_size]
        values = kv[first : first + CHUNK_PAGES, :, head_dim:].reshape(CHUNK_PAGES * page_size, head_dim)
        num = num + jnp.dot(w.astype(BF16), values, preferred_element_type=F32)
    fresh_w = jnp.exp(fresh - top)
    den = jnp.sum(den, axis=1, keepdims=True) + fresh_w
    num = num + fresh_w.astype(BF16).astype(F32) * new_value
    out = (num / den).astype(BF16)
    return jnp.concatenate([out[g * requests : (g + 1) * requests] for g in range(groups)], axis=1)


def pack_slots(routes, pages, slots):
    count = pages.shape[0]
    heads, cap = slots.shape[:2]
    dest = [routes[j] for j in range(count)]
    rank = []
    for j in range(count):
        r = jnp.int32(0)
        for i in range(j):
            r = r + (dest[i] == dest[j]).astype(jnp.int32)
        rank.append(r)
    key = [dest[j] * cap + rank[j] for j in range(count)]
    for h in range(heads):
        for k in range(cap):
            index, found = jnp.int32(0), jnp.int32(0)
            for j in range(count):
                hit = (key[j] == h * cap + k).astype(jnp.int32)
                index = index + hit * j
                found = found + hit
            page = pages[index]
            slots[h, k] = jnp.where(found > 0, page, jnp.zeros_like(page))


def kernel(
    chips,
    q_in,
    new_in,
    counts_in,
    fill_in,
    order_in,
    routes_in,
    kv_in,
    hidden_in,
    weight_in,
    pages_in,
    arr,
    blocks,
    q_ref,
    new_ref,
    counts_ref,
    fill_ref,
    order_ref,
    routes_ref,
    kv,
    weight,
    hidden,
    pages,
    slots,
    scores,
    part,
    sibling_part,
    give,
    got_pair,
    terms,
    got_terms,
    load_sem,
    own_sem,
    page_send,
    near_sem,
    far_send,
    far_sem,
    partner_sem,
    core_send,
    core_sem,
    part_send,
    part_sem,
    pair_send,
    pair_sem,
    term_send,
    term_sem,
    block_send,
    block_near,
    block_relay,
    block_far,
    block_partner,
    share_send,
    share_sem,
    wave_two,
    wave_four,
):
    pairs = chips // 2
    reach = pairs // 2
    near = 2 * reach - 1
    cap = slots.shape[1]
    block = blocks.shape[3]
    a = lax.axis_index("heads")
    z, c = a // CORES, a % CORES
    pair, parity = z // 2, z % 2
    partner_z = z + 1 - 2 * parity
    sibling = z * CORES + (1 - c)

    def lane(zt):
        return zt * CORES + c

    def remote(src, dst, send, recv, dev):
        return pltpu.make_async_remote_copy(
            src_ref=src, dst_ref=dst, send_sem=send, recv_sem=recv, device_id={"heads": dev}, device_id_type=MESH
        )

    def chip_of(k, side):
        return 2 * ((pair + pairs + k) % pairs) + side

    def signal(sem, dev):
        pl.semaphore_signal(sem, inc=1, device_id={"heads": dev}, device_id_type=MESH)

    barrier = pltpu.get_barrier_semaphore()
    signal(barrier, sibling)
    signal(barrier, lane(partner_z))
    for k in (-1, 1):
        for side in (0, 1):
            signal(barrier, lane(chip_of(k, side)))

    own_column = pl.multiple_of((c * chips + z) * block, block)
    loads = {
        name: pltpu.make_async_copy(src, dst, load_sem.at[i])
        for i, (name, src, dst) in enumerate(
            (
                ("routes", routes_in, routes_ref),
                ("pages", pages_in, pages),
                ("q", q_in, q_ref),
                ("new", new_in, new_ref),
                ("counts", counts_in, counts_ref),
                ("fill", fill_in, fill_ref),
                ("order", order_in, order_ref),
                ("kv", kv_in, kv),
                ("weight", weight_in, weight),
                ("hidden", hidden_in.at[:, pl.ds(own_column, block)], hidden),
            )
        )
    }
    for copy in loads.values():
        copy.start()
    loads["routes"].wait()
    loads["pages"].wait()
    pack_slots(routes_ref, pages, slots)
    pl.semaphore_wait(barrier, 6)

    def wave(sem, k):
        signal(sem, lane(chip_of(k, parity)))
        signal(sem, lane(chip_of(-k, parity)))


    started = []

    def go(copy):
        copy.start()
        started.append(copy)

    own = pltpu.make_async_copy(slots.at[pair], arr.at[a], own_sem)
    own.start()
    go(remote(slots.at[pair], arr.at[a], page_send.at[0], partner_sem, lane(partner_z)))

    def toward(k):
        h = (pair + pairs + (1 - 2 * parity) * k) % pairs
        to = lane(2 * h + parity)
        go(remote(slots.at[h], arr.at[a], page_send.at[2 * k - 1], near_sem.at[(k - 1) * 2 + parity], to))

    def away(k):
        h = (pair + pairs - (1 - 2 * parity) * k) % pairs
        to = lane(2 * h + 1 - parity)
        go(remote(slots.at[h], arr.at[a], page_send.at[2 * k], near_sem.at[(k - 1) * 2 + parity], to))

    def opposite():
        h = (pair + reach) % pairs
        for k in range(cap):
            m = near - 1 + k
            to = lane(2 * h + 1 - parity)
            go(remote(slots.at[h, k], arr.at[a, k], page_send.at[m + 1], near_sem.at[m], to))

    def source(m, side):
        if m >= near - 1:
            return 2 * ((pair + reach) % pairs) + 1 - side
        k, sp = m // 2 + 1, m % 2
        return 2 * ((pair + pairs + (2 * side - 1) * k) % pairs) + sp

    def arrived(m, side):
        row = arr.at[lane(source(m, side))]
        return row.at[m - near + 1] if m >= near - 1 else row

    def to_sibling(zs):
        row = arr.at[lane(zs)]
        go(remote(row, row, core_send.at[zs], core_sem.at[zs], sibling))

    last_page = near + cap - 2

    def relay_near(m):
        pages_ref = arrived(m, parity)
        remote(pages_ref, pages_ref, far_send.at[m], near_sem.at[m], lane(partner_z)).wait_recv()
        go(remote(pages_ref, pages_ref, far_send.at[m], far_sem.at[m], lane(partner_z)))
        if m < near - 1 or m == last_page:
            to_sibling(source(m, parity))

    def take_far(m):
        pages_ref = arrived(m, 1 - parity)
        remote(pages_ref, pages_ref, far_send.at[m], far_sem.at[m], lane(partner_z)).wait_recv()
        if m < near - 1 or m == last_page:
            to_sibling(source(m, 1 - parity))

    exchange = remote(part.at[1 - c], sibling_part, part_send, part_sem, sibling)
    share = remote(blocks.at[c], blocks.at[c], share_send, share_sem, sibling)

    state = {}

    def attention_scores():
        for name in ("q", "new", "counts", "fill", "order"):
            loads[name].wait()
        limits = page_limits(counts_ref, fill_ref, order_ref, kv.shape[1])
        loads["kv"].wait()
        state["top"], state["fresh"] = attend_scores(q_ref, new_ref, kv, scores, limits)

    def attention():
        attn = attend_values(q_ref, new_ref, kv, scores, state["top"], state["fresh"])
        loads["weight"].wait()
        for half in range(CORES):

            def project(zz, _, half=half):
                columns = pl.ds(pl.multiple_of((half * chips + zz) * block, block), block)
                part[half, zz] = jnp.dot(attn, weight[:, columns], preferred_element_type=F32)
                return 0

            lax.fori_loop(0, chips, project, 0, unroll=4)
        own.wait()
        to_sibling(z)
        exchange.start()

    turned = (z + chips - 1) % chips
    team, side_here = turned // 2, turned % 2

    def member(k, side):
        return (2 * ((team + pairs + k) % pairs) + side + 1) % chips

    mate = lane(member(0, 1 - side_here))
    mate_z = member(0, 1 - side_here)

    def owner(m, side):
        if m == near - 1:
            return member(reach, 1 - side)
        return member((2 * side - 1) * (m // 2 + 1), m % 2)

    def core_sum(zt):
        return part[c, zt] + sibling_part[zt]

    pair_exchange = remote(give, got_pair, pair_send, pair_sem, mate)

    def send_terms():
        exchange.wait_recv()
        for m in range(near):
            give[m] = core_sum(owner(m, 1 - side_here)).astype(BF16)
        give[near] = core_sum(mate_z).astype(BF16)
        pair_exchange.start()

    def send_pair_terms():
        pair_exchange.wait_recv()
        for m in range(near):
            terms[m] = (core_sum(owner(m, side_here)) + got_pair[m].astype(F32)).astype(BF16)
        for m in range(near):
            place = near - 1 if m == near - 1 else (1 - side_here) * (reach - 1) + m // 2
            to = lane(owner(m, side_here))
            go(remote(terms.at[m], got_terms.at[place], term_send.at[m], term_sem.at[place], to))

    def sum_terms():
        total = core_sum(z) + got_pair[near].astype(F32)
        for m in range(near):
            remote(terms.at[m], got_terms.at[m], term_send.at[m], term_sem.at[m], sibling).wait_recv()
            total = total + got_terms[m].astype(F32)
        loads["hidden"].wait()
        blocks[c, z] = (hidden[...].astype(F32) + total).astype(BF16)

    def send_block():
        mine = blocks.at[c, z]
        go(remote(mine, mine, block_send.at[near], block_partner, mate))
        for m in range(near):
            k = m // 2 + 1
            if m == near - 1:
                at, zt = near - 1, member(reach, 1 - side_here)
            elif m % 2 == 0:
                at, zt = (k - 1) * 2 + side_here, member(k, 0)
            else:
                at, zt = (k - 1) * 2 + side_here, member(-k, 1)
            go(remote(mine, mine, block_send.at[m], block_near.at[at], lane(zt)))

    def relay_blocks():
        for m in range(near):
            theirs = blocks.at[c, owner(m, side_here)]
            remote(theirs, theirs, block_relay.at[m], block_near.at[m], sibling).wait_recv()
            go(remote(theirs, theirs, block_relay.at[m], block_far.at[m], mate))

    def share_blocks():
        theirs = blocks.at[c, mate_z]
        remote(theirs, theirs, block_send.at[near], block_partner, sibling).wait_recv()
        for m in range(near):
            theirs = blocks.at[c, owner(m, 1 - side_here)]
            remote(theirs, theirs, block_relay.at[m], block_far.at[m], sibling).wait_recv()
        share.start()

    def shared():
        remote(blocks.at[1 - c], blocks.at[1 - c], share_send, share_sem, sibling).wait_recv()

    def take_partner():
        row = arr.at[lane(partner_z)]
        remote(row, row, page_send.at[0], partner_sem, sibling).wait_recv()
        to_sibling(partner_z)

    named = {
        "scores": attention_scores,
        "attention": attention,
        "tell2": lambda: wave(wave_two, 1),
        "know2": lambda: pl.semaphore_wait(wave_two, 2),
        "tell4": lambda: wave(wave_four, 2),
        "know4": lambda: pl.semaphore_wait(wave_four, 2),
        "terms": send_terms,
        "pair": send_pair_terms,
        "brelay": relay_blocks,
        "sum": sum_terms,
        "block": send_block,
        "share": share_blocks,
        "shared": shared,
        "partner": take_partner,
        "opposite": opposite,
    }
    numbered = {"toward": toward, "away": away, "relay": relay_near, "far": take_far}
    for step in PLAN:
        if step in named:
            named[step]()
        else:
            word = step.rstrip("0123456789")
            numbered[word](int(step[len(word) :]))

    for i in range(chips):
        theirs = arr.at[i * CORES + 1 - c]
        remote(theirs, theirs, core_send.at[i], core_sem.at[i], sibling).wait_recv()
    exchange.wait_send()
    pair_exchange.wait_send()
    share.wait_send()
    for copy in started:
        copy.wait_send()


def finish_kernel(arr, blocks, gain_in, arrival, residual_out, normed_out, gain_ref, gain_wide, residual, normed, sem):
    parts = ARRIVAL_COPIES
    rows = arr.shape[0] // parts
    copies = [
        pltpu.make_async_copy(arr.at[pl.ds(i * rows, rows)], arrival.at[pl.ds(i * rows, rows)], sem.at[i])
        for i in range(parts)
    ]
    gain_copy = pltpu.make_async_copy(gain_in, gain_ref, sem.at[parts])
    gain_copy.start()
    for copy in copies:
        copy.start()
    halves, chips, requests, block = blocks.shape

    def squares(b, acc):
        x = blocks[b // chips, b % chips].astype(F32)
        return acc + x * x

    acc = lax.fori_loop(0, halves * chips, squares, jnp.zeros((requests, block), F32), unroll=8)
    width = halves * chips * block
    inverse = lax.rsqrt(jnp.sum(acc, axis=1, keepdims=True) / width + norm_epsilon)
    gain_copy.wait()
    gain_wide[...] = gain_ref[...].astype(F32)
    per_block = block // gain_wide.shape[1]

    def normalise(b, _):
        columns = pl.ds(pl.multiple_of(b * block, block), block)
        x = blocks[b // chips, b % chips]
        gain = jnp.concatenate([gain_wide[pl.ds(b * per_block + i, 1), :] for i in range(per_block)], axis=1)
        residual[:, columns] = x
        normed[:, columns] = (x.astype(F32) * inverse * gain).astype(BF16)
        return 0

    lax.fori_loop(0, halves * chips, normalise, 0, unroll=8)
    copies.append(pltpu.make_async_copy(residual, residual_out, sem.at[parts + 1]))
    copies.append(pltpu.make_async_copy(normed, normed_out, sem.at[parts + 2]))
    copies[-2].start()
    copies[-1].start()
    for copy in copies:
        copy.wait()


def per_device(
    queries,
    new_kv,
    kv_pool,
    page_counts,
    last_fill,
    page_order,
    hidden,
    out_weight,
    norm_gain,
    sectioned,
    routes,
):
    head_count = lax.axis_size("heads")
    chips = head_count // CORES
    requests, width = hidden.shape
    _, pool, page_size, kv_width = kv_pool.shape
    page_count = sectioned.shape[2]
    block = width // head_count
    pairs = chips // 2
    near = pairs - 1
    if pairs != KV_HEADS or pairs != 8 or new_kv.shape[0] != 1:
        raise ValueError("unexpected layout")
    vmem = pl.BlockSpec(memory_space=pltpu.VMEM)
    hbm = pl.BlockSpec(memory_space=pltpu.HBM)
    anywhere = pl.BlockSpec(memory_space=pl.ANY)
    dma = pltpu.SemaphoreType.DMA
    slot_shape = (PER_HEAD_CAP, page_size, kv_width)
    landed, blocks = pl.pallas_call(
        functools.partial(kernel, chips),
        out_shape=(
            pltpu.VMEM((head_count, *slot_shape), BF16),
            pltpu.VMEM((CORES, chips, requests, block), BF16),
        ),
        in_specs=[hbm] * 10,
        out_specs=(anywhere, vmem),
        scratch_shapes=[
            pltpu.VMEM(queries.shape, BF16),
            pltpu.VMEM(new_kv.shape[1:], BF16),
            pltpu.VMEM(page_counts.shape, jnp.int32),
            pltpu.VMEM(last_fill.shape, jnp.int32),
            pltpu.VMEM(page_order.shape, jnp.int32),
            pltpu.SMEM((page_count,), jnp.int32),
            pltpu.VMEM((pool, page_size, kv_width), BF16),
            pltpu.VMEM(out_weight.shape, BF16),
            pltpu.VMEM((requests, block), BF16),
            pltpu.VMEM((page_count, page_size, kv_width), BF16),
            pltpu.VMEM((KV_HEADS, *slot_shape), BF16),
            pltpu.VMEM((requests * queries.shape[1] * 2 // kv_width, pool * page_size), F32),
            pltpu.VMEM((CORES, chips, requests, block), F32),
            pltpu.VMEM((chips, requests, block), F32),
            pltpu.VMEM((near + 1, requests, block), BF16),
            pltpu.VMEM((near + 1, requests, block), BF16),
            pltpu.VMEM((near, requests, block), BF16),
            pltpu.VMEM((near, requests, block), BF16),
            dma((10,)),
            dma,
            dma((near + PER_HEAD_CAP,)),
            dma((near - 1 + PER_HEAD_CAP,)),
            dma((near - 1 + PER_HEAD_CAP,)),
            dma((near - 1 + PER_HEAD_CAP,)),
            dma,
            dma((chips,)),
            dma((chips,)),
            dma,
            dma,
            dma,
            dma,
            dma((near,)),
            dma((near,)),
            dma((near + 1,)),
            dma((near,)),
            dma((near,)),
            dma((near,)),
            dma,
            dma,
            dma,
            pltpu.SemaphoreType.REGULAR,
            pltpu.SemaphoreType.REGULAR,
        ],
        compiler_params=pltpu.CompilerParams(
            collective_id=0, has_side_effects=True, vmem_limit_bytes=40 * 1024 * 1024
        ),
    )(*[pltpu.with_memory_space_constraint(x, pltpu.HBM) for x in (
        queries,
        new_kv[0],
        page_counts,
        last_fill,
        page_order,
        routes.reshape(page_count),
        kv_pool[0],
        hidden,
        out_weight,
        sectioned[0, 0],
    )])
    arrival, residual, normed = pl.pallas_call(
        finish_kernel,
        out_shape=(
            jax.ShapeDtypeStruct((head_count, *slot_shape), BF16),
            jax.ShapeDtypeStruct((requests, width), BF16),
            jax.ShapeDtypeStruct((requests, width), BF16),
        ),
        in_specs=[vmem, vmem, hbm],
        out_specs=(hbm, hbm, hbm),
        scratch_shapes=[
            pltpu.VMEM((width // LANES, LANES), BF16),
            pltpu.VMEM((width // LANES, LANES), F32),
            pltpu.VMEM((requests, width), BF16),
            pltpu.VMEM((requests, width), BF16),
            dma((ARRIVAL_COPIES + 3,)),
        ],
        compiler_params=pltpu.CompilerParams(vmem_limit_bytes=16 * 1024 * 1024),
    )(
        landed,
        blocks,
        pltpu.with_memory_space_constraint(norm_gain.reshape(width // LANES, LANES), pltpu.HBM),
    )
    return (residual, normed, arrival[None, None])


def solution(mesh):
    return jax.shard_map(
        per_device,
        mesh=mesh,
        in_specs=(
            P(("groups", "batch"), "heads"),
            P(("groups", "heads"), "batch", None),
            P(("groups", "heads"), "batch", None, None),
            P(("groups", "batch"), None),
            P(("groups", "batch"), None),
            P(("groups", "batch"), None),
            P(("groups", "batch"), None),
            P("heads", None),
            P(),
            P(("groups", "heads"), "batch", None, None, None),
            P(("groups", "heads"), "batch", None, None),
        ),
        out_specs=(
            P(("groups", "batch"), None),
            P(("groups", "batch"), None),
            P(("groups", "heads"), "batch", None, None, None, None),
        ),
        check_vma=False,
    )
```

```python
import functools

import jax
import jax.numpy as jnp
from jax import lax
from jax.experimental import pallas as pl
from jax.experimental.pallas import tpu as pltpu
from jax.sharding import PartitionSpec as P

KV_HEADS = 8
PER_HEAD_CAP = 2
CORES = 2
CHUNK_PAGES = 8
LANES = 128
ARRIVAL_COPIES = 4
PLAN = (
    "away1",
    "toward1",
    "tell2",
    "scores",
    "know2",
    "away2",
    "toward2",
    "tell4",
    "attention",
    "know4",
    "terms",
    "away3",
    "relay0",
    "relay1",
    "partner",
    "pair",
    "toward3",
    "relay2",
    "relay3",
    "opposite",
    "sum",
    "block",
    "relay4",
    "relay5",
    "relay6",
    "relay7",
    "brelay",
    "brelast",
    "far0",
    "far1",
    "far2",
    "far3",
    "share",
    "shared",
    "far4",
    "far5",
    "far6",
    "far7",
)
norm_epsilon = 1e-06

MESH = pl.DeviceIdType.MESH
F32 = jnp.float32
BF16 = jnp.bfloat16


def page_limits(counts_ref, fill_ref, order_ref, page_size):
    requests, pool = counts_ref.shape[1], order_ref.shape[1]
    lane = lax.broadcasted_iota(jnp.int32, (requests, requests), 1)
    row = lax.broadcasted_iota(jnp.int32, (requests, requests), 0)
    counts = jnp.broadcast_to(counts_ref[...].astype(F32), (requests, requests))
    fill = jnp.broadcast_to(fill_ref[...].astype(F32), (requests, requests))
    count_col = jnp.sum(jnp.where(lane == row, counts, 0.0), axis=1, keepdims=True)
    fill_col = jnp.sum(jnp.where(lane == row, fill, 0.0), axis=1, keepdims=True)
    ends = jnp.sum(jnp.where(lane <= row, counts, 0.0), axis=1, keepdims=True)
    starts = ends - count_col
    context = (count_col - 1.0) * page_size + fill_col
    place = lax.broadcasted_iota(jnp.int32, (requests, 128), 1).astype(F32)
    live = jnp.clip(context - page_size * (place - starts), 0.0, float(page_size))
    live = jnp.where((place >= starts) & (place < ends), live, 0.0)
    order = jnp.broadcast_to(order_ref[...], (pool, pool))
    lane = lax.broadcasted_iota(jnp.int32, (pool, pool), 1)
    row = lax.broadcasted_iota(jnp.int32, (pool, pool), 0)
    order_col = jnp.sum(jnp.where(lane == row, order.astype(F32), 0.0), axis=1, keepdims=True)
    page = lax.broadcasted_iota(jnp.int32, (pool, 128), 1).astype(F32)
    one_hot = jnp.where(order_col == page, 1.0, 0.0).astype(BF16)
    return jnp.dot(live[:, :pool].astype(BF16), one_hot, preferred_element_type=F32)


def attend_scores(q_ref, new_ref, kv, scores, limits):
    pool, page_size, width = kv.shape
    head_dim = width // 2
    requests = q_ref.shape[0]
    groups = q_ref.shape[1] // head_dim
    scale = 1.0 / head_dim**0.5
    q = jnp.concatenate([q_ref[:, g * head_dim : (g + 1) * head_dim] for g in range(groups)], axis=0)
    limits = jnp.concatenate([limits] * groups, axis=0)
    rows = groups * requests
    new_key = jnp.concatenate([new_ref[:, :head_dim].astype(F32)] * groups, axis=0)
    fresh = jnp.sum(q.astype(F32) * new_key, axis=1, keepdims=True) * scale
    token = lax.broadcasted_iota(jnp.int32, (rows, page_size), 1).astype(F32)
    top = jnp.full((rows, page_size), -1e30, F32)
    for first in range(0, pool, CHUNK_PAGES):
        keys = kv[first : first + CHUNK_PAGES, :, :head_dim].reshape(CHUNK_PAGES * page_size, head_dim)
        s = lax.dot_general(q, keys, (((1,), (1,)), ((), ())), preferred_element_type=F32) * scale
        for i in range(CHUNK_PAGES):
            part = s[:, i * page_size : (i + 1) * page_size]
            part = jnp.where(token < limits[:, first + i : first + i + 1], part, -1e30)
            top = jnp.maximum(top, part)
            scores[:, (first + i) * page_size : (first + i + 1) * page_size] = part
    return jnp.maximum(jnp.max(top, axis=1, keepdims=True), fresh), fresh


def attend_values(q_ref, new_ref, kv, scores, top, fresh):
    pool, page_size, width = kv.shape
    head_dim = width // 2
    requests = q_ref.shape[0]
    groups = q_ref.shape[1] // head_dim
    rows = groups * requests
    new_value = jnp.concatenate([new_ref[:, head_dim:].astype(F32)] * groups, axis=0)
    den = jnp.zeros((rows, page_size), F32)
    num = jnp.zeros((rows, head_dim), F32)
    for first in range(0, pool, CHUNK_PAGES):
        cols = slice(first * page_size, (first + CHUNK_PAGES) * page_size)
        w = jnp.exp(scores[:, cols] - top)
        for i in range(CHUNK_PAGES):
            den = den + w[:, i * page_size : (i + 1) * page_size]
        values = kv[first : first + CHUNK_PAGES, :, head_dim:].reshape(CHUNK_PAGES * page_size, head_dim)
        num = num + jnp.dot(w.astype(BF16), values, preferred_element_type=F32)
    fresh_w = jnp.exp(fresh - top)
    den = jnp.sum(den, axis=1, keepdims=True) + fresh_w
    num = num + fresh_w.astype(BF16).astype(F32) * new_value
    out = (num / den).astype(BF16)
    return jnp.concatenate([out[g * requests : (g + 1) * requests] for g in range(groups)], axis=1)


def pack_slots(routes, pages, slots):
    count = pages.shape[0]
    heads, cap = slots.shape[:2]
    dest = [routes[j] for j in range(count)]
    rank = []
    for j in range(count):
        r = jnp.int32(0)
        for i in range(j):
            r = r + (dest[i] == dest[j]).astype(jnp.int32)
        rank.append(r)
    key = [dest[j] * cap + rank[j] for j in range(count)]
    for h in range(heads):
        for k in range(cap):
            index, found = jnp.int32(0), jnp.int32(0)
            for j in range(count):
                hit = (key[j] == h * cap + k).astype(jnp.int32)
                index = index + hit * j
                found = found + hit
            page = pages[index]
            slots[h, k] = jnp.where(found > 0, page, jnp.zeros_like(page))


def kernel(
    chips,
    q_in,
    new_in,
    counts_in,
    fill_in,
    order_in,
    routes_in,
    kv_in,
    hidden_in,
    weight_in,
    pages_in,
    arr,
    blocks,
    q_ref,
    new_ref,
    counts_ref,
    fill_ref,
    order_ref,
    routes_ref,
    kv,
    weight,
    hidden,
    pages,
    slots,
    scores,
    part,
    sibling_part,
    give,
    got_pair,
    terms,
    got_terms,
    load_sem,
    own_sem,
    page_send,
    near_sem,
    far_send,
    far_sem,
    partner_sem,
    core_send,
    core_sem,
    part_send,
    part_sem,
    pair_send,
    pair_sem,
    term_send,
    term_sem,
    block_send,
    block_near,
    block_relay,
    block_far,
    block_partner,
    share_send,
    share_sem,
    wave_two,
    wave_four,
):
    pairs = chips // 2
    reach = pairs // 2
    near = 2 * reach - 1
    cap = slots.shape[1]
    block = blocks.shape[3]
    a = lax.axis_index("heads")
    z, c = a // CORES, a % CORES
    pair, parity = z // 2, z % 2
    partner_z = z + 1 - 2 * parity
    sibling = z * CORES + (1 - c)

    def lane(zt):
        return zt * CORES + c

    def remote(src, dst, send, recv, dev):
        return pltpu.make_async_remote_copy(
            src_ref=src, dst_ref=dst, send_sem=send, recv_sem=recv, device_id={"heads": dev}, device_id_type=MESH
        )

    def chip_of(k, side):
        return 2 * ((pair + pairs + k) % pairs) + side

    def signal(sem, dev):
        pl.semaphore_signal(sem, inc=1, device_id={"heads": dev}, device_id_type=MESH)

    barrier = pltpu.get_barrier_semaphore()
    signal(barrier, sibling)
    signal(barrier, lane(partner_z))
    for k in (-1, 1):
        for side in (0, 1):
            signal(barrier, lane(chip_of(k, side)))

    own_column = pl.multiple_of((c * chips + z) * block, block)
    loads = {
        name: pltpu.make_async_copy(src, dst, load_sem.at[i])
        for i, (name, src, dst) in enumerate(
            (
                ("routes", routes_in, routes_ref),
                ("pages", pages_in, pages),
                ("q", q_in, q_ref),
                ("new", new_in, new_ref),
                ("counts", counts_in, counts_ref),
                ("fill", fill_in, fill_ref),
                ("order", order_in, order_ref),
                ("kv", kv_in, kv),
                ("weight", weight_in, weight),
                ("hidden", hidden_in.at[:, pl.ds(own_column, block)], hidden),
            )
        )
    }
    for copy in loads.values():
        copy.start()
    loads["routes"].wait()
    loads["pages"].wait()
    pack_slots(routes_ref, pages, slots)
    pl.semaphore_wait(barrier, 6)

    def wave(sem, k):
        signal(sem, lane(chip_of(k, parity)))
        signal(sem, lane(chip_of(-k, parity)))


    started = []

    def go(copy):
        copy.start()
        started.append(copy)

    own = pltpu.make_async_copy(slots.at[pair], arr.at[a], own_sem)
    own.start()
    go(remote(slots.at[pair], arr.at[a], page_send.at[0], partner_sem, lane(partner_z)))

    def toward(k):
        h = (pair + pairs + (1 - 2 * parity) * k) % pairs
        to = lane(2 * h + parity)
        go(remote(slots.at[h], arr.at[a], page_send.at[2 * k - 1], near_sem.at[(k - 1) * 2 + parity], to))

    def away(k):
        h = (pair + pairs - (1 - 2 * parity) * k) % pairs
        to = lane(2 * h + 1 - parity)
        go(remote(slots.at[h], arr.at[a], page_send.at[2 * k], near_sem.at[(k - 1) * 2 + parity], to))

    def opposite():
        h = (pair + reach) % pairs
        for k in range(cap):
            m = near - 1 + k
            to = lane(2 * h + 1 - parity)
            go(remote(slots.at[h, k], arr.at[a, k], page_send.at[m + 1], near_sem.at[m], to))

    def source(m, side):
        if m >= near - 1:
            return 2 * ((pair + reach) % pairs) + 1 - side
        k, sp = m // 2 + 1, m % 2
        return 2 * ((pair + pairs + (2 * side - 1) * k) % pairs) + sp

    def arrived(m, side):
        row = arr.at[lane(source(m, side))]
        return row.at[m - near + 1] if m >= near - 1 else row

    def to_sibling(zs):
        row = arr.at[lane(zs)]
        go(remote(row, row, core_send.at[zs], core_sem.at[zs], sibling))

    last_page = near + cap - 2

    def relay_near(m):
        pages_ref = arrived(m, parity)
        remote(pages_ref, pages_ref, far_send.at[m], near_sem.at[m], lane(partner_z)).wait_recv()
        go(remote(pages_ref, pages_ref, far_send.at[m], far_sem.at[m], lane(partner_z)))
        if m < near - 1 or m == last_page:
            to_sibling(source(m, parity))

    def take_far(m):
        pages_ref = arrived(m, 1 - parity)
        remote(pages_ref, pages_ref, far_send.at[m], far_sem.at[m], lane(partner_z)).wait_recv()
        if m < near - 1 or m == last_page:
            to_sibling(source(m, 1 - parity))

    exchange = remote(part.at[1 - c], sibling_part, part_send, part_sem, sibling)
    share = remote(blocks.at[c], blocks.at[c], share_send, share_sem, sibling)

    state = {}

    def attention_scores():
        for name in ("q", "new", "counts", "fill", "order"):
            loads[name].wait()
        limits = page_limits(counts_ref, fill_ref, order_ref, kv.shape[1])
        loads["kv"].wait()
        state["top"], state["fresh"] = attend_scores(q_ref, new_ref, kv, scores, limits)

    def attention():
        attn = attend_values(q_ref, new_ref, kv, scores, state["top"], state["fresh"])
        loads["weight"].wait()
        for half in range(CORES):

            def project(zz, _, half=half):
                columns = pl.ds(pl.multiple_of((half * chips + zz) * block, block), block)
                part[half, zz] = jnp.dot(attn, weight[:, columns], preferred_element_type=F32)
                return 0

            lax.fori_loop(0, chips, project, 0, unroll=4)
        own.wait()
        to_sibling(z)
        exchange.start()

    turned = (z + chips - 1) % chips
    team, side_here = turned // 2, turned % 2

    def member(k, side):
        return (2 * ((team + pairs + k) % pairs) + side + 1) % chips

    mate = lane(member(0, 1 - side_here))
    mate_z = member(0, 1 - side_here)

    def owner(m, side):
        if m == near - 1:
            return member(reach, 1 - side)
        return member((2 * side - 1) * (m // 2 + 1), m % 2)

    def core_sum(zt):
        return part[c, zt] + sibling_part[zt]

    pair_exchange = remote(give, got_pair, pair_send, pair_sem, mate)

    def send_terms():
        exchange.wait_recv()
        for m in range(near):
            give[m] = core_sum(owner(m, 1 - side_here)).astype(BF16)
        give[near] = core_sum(mate_z).astype(BF16)
        pair_exchange.start()

    def send_pair_terms():
        pair_exchange.wait_recv()
        for m in range(near):
            terms[m] = (core_sum(owner(m, side_here)) + got_pair[m].astype(F32)).astype(BF16)
        for m in range(near):
            place = near - 1 if m == near - 1 else (1 - side_here) * (reach - 1) + m // 2
            to = lane(owner(m, side_here))
            go(remote(terms.at[m], got_terms.at[place], term_send.at[m], term_sem.at[place], to))

    def sum_terms():
        total = core_sum(z) + got_pair[near].astype(F32)
        for m in range(near):
            remote(terms.at[m], got_terms.at[m], term_send.at[m], term_sem.at[m], sibling).wait_recv()
            total = total + got_terms[m].astype(F32)
        loads["hidden"].wait()
        blocks[c, z] = (hidden[...].astype(F32) + total).astype(BF16)

    def send_block():
        mine = blocks.at[c, z]
        go(remote(mine, mine, block_send.at[near], block_partner, mate))
        for m in range(near):
            k = m // 2 + 1
            if m == near - 1:
                at, zt = near - 1, member(reach, 1 - side_here)
            elif m % 2 == 0:
                at, zt = (k - 1) * 2 + side_here, member(k, 0)
            else:
                at, zt = (k - 1) * 2 + side_here, member(-k, 1)
            go(remote(mine, mine, block_send.at[m], block_near.at[at], lane(zt)))

    def relay_blocks(arrivals):
        for m in arrivals:
            theirs = blocks.at[c, owner(m, side_here)]
            remote(theirs, theirs, block_relay.at[m], block_near.at[m], sibling).wait_recv()
            go(remote(theirs, theirs, block_relay.at[m], block_far.at[m], mate))

    def share_blocks():
        theirs = blocks.at[c, mate_z]
        remote(theirs, theirs, block_send.at[near], block_partner, sibling).wait_recv()
        for m in range(near):
            theirs = blocks.at[c, owner(m, 1 - side_here)]
            remote(theirs, theirs, block_relay.at[m], block_far.at[m], sibling).wait_recv()
        share.start()

    def shared():
        remote(blocks.at[1 - c], blocks.at[1 - c], share_send, share_sem, sibling).wait_recv()

    def take_partner():
        row = arr.at[lane(partner_z)]
        remote(row, row, page_send.at[0], partner_sem, sibling).wait_recv()
        to_sibling(partner_z)

    named = {
        "scores": attention_scores,
        "attention": attention,
        "tell2": lambda: wave(wave_two, 1),
        "know2": lambda: pl.semaphore_wait(wave_two, 2),
        "tell4": lambda: wave(wave_four, 2),
        "know4": lambda: pl.semaphore_wait(wave_four, 2),
        "terms": send_terms,
        "pair": send_pair_terms,
        "brelay": lambda: relay_blocks(range(4)),
        "brelast": lambda: relay_blocks(range(4, near)),
        "sum": sum_terms,
        "block": send_block,
        "share": share_blocks,
        "shared": shared,
        "partner": take_partner,
        "opposite": opposite,
    }
    numbered = {"toward": toward, "away": away, "relay": relay_near, "far": take_far}
    for step in PLAN:
        if step in named:
            named[step]()
        else:
            word = step.rstrip("0123456789")
            numbered[word](int(step[len(word) :]))

    for i in range(chips):
        theirs = arr.at[i * CORES + 1 - c]
        remote(theirs, theirs, core_send.at[i], core_sem.at[i], sibling).wait_recv()
    exchange.wait_send()
    pair_exchange.wait_send()
    share.wait_send()
    for copy in started:
        copy.wait_send()


def finish_kernel(arr, blocks, gain_in, arrival, residual_out, normed_out, gain_ref, gain_wide, residual, normed, sem):
    parts = ARRIVAL_COPIES
    rows = arr.shape[0] // parts
    copies = [
        pltpu.make_async_copy(arr.at[pl.ds(i * rows, rows)], arrival.at[pl.ds(i * rows, rows)], sem.at[i])
        for i in range(parts)
    ]
    gain_copy = pltpu.make_async_copy(gain_in, gain_ref, sem.at[parts])
    gain_copy.start()
    for copy in copies:
        copy.start()
    halves, chips, requests, block = blocks.shape

    def squares(b, acc):
        x = blocks[b // chips, b % chips].astype(F32)
        return acc + x * x

    acc = lax.fori_loop(0, halves * chips, squares, jnp.zeros((requests, block), F32), unroll=8)
    width = halves * chips * block
    inverse = lax.rsqrt(jnp.sum(acc, axis=1, keepdims=True) / width + norm_epsilon)
    gain_copy.wait()
    gain_wide[...] = gain_ref[...].astype(F32)
    per_block = block // gain_wide.shape[1]

    def normalise(b, _):
        columns = pl.ds(pl.multiple_of(b * block, block), block)
        x = blocks[b // chips, b % chips]
        gain = jnp.concatenate([gain_wide[pl.ds(b * per_block + i, 1), :] for i in range(per_block)], axis=1)
        residual[:, columns] = x
        normed[:, columns] = (x.astype(F32) * inverse * gain).astype(BF16)
        return 0

    lax.fori_loop(0, halves * chips, normalise, 0, unroll=8)
    copies.append(pltpu.make_async_copy(residual, residual_out, sem.at[parts + 1]))
    copies.append(pltpu.make_async_copy(normed, normed_out, sem.at[parts + 2]))
    copies[-2].start()
    copies[-1].start()
    for copy in copies:
        copy.wait()


def per_device(
    queries,
    new_kv,
    kv_pool,
    page_counts,
    last_fill,
    page_order,
    hidden,
    out_weight,
    norm_gain,
    sectioned,
    routes,
):
    head_count = lax.axis_size("heads")
    chips = head_count // CORES
    requests, width = hidden.shape
    _, pool, page_size, kv_width = kv_pool.shape
    page_count = sectioned.shape[2]
    block = width // head_count
    pairs = chips // 2
    near = pairs - 1
    if pairs != KV_HEADS or pairs != 8 or new_kv.shape[0] != 1:
        raise ValueError("unexpected layout")
    vmem = pl.BlockSpec(memory_space=pltpu.VMEM)
    hbm = pl.BlockSpec(memory_space=pltpu.HBM)
    anywhere = pl.BlockSpec(memory_space=pl.ANY)
    dma = pltpu.SemaphoreType.DMA
    slot_shape = (PER_HEAD_CAP, page_size, kv_width)
    landed, blocks = pl.pallas_call(
        functools.partial(kernel, chips),
        out_shape=(
            pltpu.VMEM((head_count, *slot_shape), BF16),
            pltpu.VMEM((CORES, chips, requests, block), BF16),
        ),
        in_specs=[hbm] * 10,
        out_specs=(anywhere, vmem),
        scratch_shapes=[
            pltpu.VMEM(queries.shape, BF16),
            pltpu.VMEM(new_kv.shape[1:], BF16),
            pltpu.VMEM(page_counts.shape, jnp.int32),
            pltpu.VMEM(last_fill.shape, jnp.int32),
            pltpu.VMEM(page_order.shape, jnp.int32),
            pltpu.SMEM((page_count,), jnp.int32),
            pltpu.VMEM((pool, page_size, kv_width), BF16),
            pltpu.VMEM(out_weight.shape, BF16),
            pltpu.VMEM((requests, block), BF16),
            pltpu.VMEM((page_count, page_size, kv_width), BF16),
            pltpu.VMEM((KV_HEADS, *slot_shape), BF16),
            pltpu.VMEM((requests * queries.shape[1] * 2 // kv_width, pool * page_size), F32),
            pltpu.VMEM((CORES, chips, requests, block), F32),
            pltpu.VMEM((chips, requests, block), F32),
            pltpu.VMEM((near + 1, requests, block), BF16),
            pltpu.VMEM((near + 1, requests, block), BF16),
            pltpu.VMEM((near, requests, block), BF16),
            pltpu.VMEM((near, requests, block), BF16),
            dma((10,)),
            dma,
            dma((near + PER_HEAD_CAP,)),
            dma((near - 1 + PER_HEAD_CAP,)),
            dma((near - 1 + PER_HEAD_CAP,)),
            dma((near - 1 + PER_HEAD_CAP,)),
            dma,
            dma((chips,)),
            dma((chips,)),
            dma,
            dma,
            dma,
            dma,
            dma((near,)),
            dma((near,)),
            dma((near + 1,)),
            dma((near,)),
            dma((near,)),
            dma((near,)),
            dma,
            dma,
            dma,
            pltpu.SemaphoreType.REGULAR,
            pltpu.SemaphoreType.REGULAR,
        ],
        compiler_params=pltpu.CompilerParams(
            collective_id=0, has_side_effects=True, vmem_limit_bytes=40 * 1024 * 1024
        ),
    )(*[pltpu.with_memory_space_constraint(x, pltpu.HBM) for x in (
        queries,
        new_kv[0],
        page_counts,
        last_fill,
        page_order,
        routes.reshape(page_count),
        kv_pool[0],
        hidden,
        out_weight,
        sectioned[0, 0],
    )])
    arrival, residual, normed = pl.pallas_call(
        finish_kernel,
        out_shape=(
            jax.ShapeDtypeStruct((head_count, *slot_shape), BF16),
            jax.ShapeDtypeStruct((requests, width), BF16),
            jax.ShapeDtypeStruct((requests, width), BF16),
        ),
        in_specs=[vmem, vmem, hbm],
        out_specs=(hbm, hbm, hbm),
        scratch_shapes=[
            pltpu.VMEM((width // LANES, LANES), BF16),
            pltpu.VMEM((width // LANES, LANES), F32),
            pltpu.VMEM((requests, width), BF16),
            pltpu.VMEM((requests, width), BF16),
            dma((ARRIVAL_COPIES + 3,)),
        ],
        compiler_params=pltpu.CompilerParams(vmem_limit_bytes=16 * 1024 * 1024),
    )(
        landed,
        blocks,
        pltpu.with_memory_space_constraint(norm_gain.reshape(width // LANES, LANES), pltpu.HBM),
    )
    return (residual, normed, arrival[None, None])


def solution(mesh):
    return jax.shard_map(
        per_device,
        mesh=mesh,
        in_specs=(
            P(("groups", "batch"), "heads"),
            P(("groups", "heads"), "batch", None),
            P(("groups", "heads"), "batch", None, None),
            P(("groups", "batch"), None),
            P(("groups", "batch"), None),
            P(("groups", "batch"), None),
            P(("groups", "batch"), None),
            P("heads", None),
            P(),
            P(("groups", "heads"), "batch", None, None, None),
            P(("groups", "heads"), "batch", None, None),
        ),
        out_specs=(
            P(("groups", "batch"), None),
            P(("groups", "batch"), None),
            P(("groups", "heads"), "batch", None, None, None, None),
        ),
        check_vma=False,
    )
```
